32 devices in a mesh: ta: 2 (over x), gz: 4 (over y, core), gy: 4 (over z).
Axes of the slice: x: 2, y: 2, z: 4, core: 2. Of those that a mesh axis runs over, the one named last changes fastest.
Arguments:
- near_null: float32 [8, 16, 16, 12, 12, 128], P('ta', 'gz', 'gy'), may hold values from -400 to 400
- offsets: int32 [4], replicated, may hold values from 1 to 3
- owner_slot: int32 [2, 4, 4, 16], P('ta', 'gz', 'gy'), may hold values from 0 to 15, each once within a row
Outputs:
- result: float32 [512, 2, 12, 6, 2, 256], P(('ta', 'gz', 'gy'))
The draws below stay inside these ranges and needn't reach their ends.
Inputs may be any that keep to these rules, and one draw needn't show every extreme that they name: The same offsets hold for every device. `owner_slot`: each device's row is a permutation of 0 to 15.
All inputs are finite; a program needn't handle non-finite values.
Results may differ from the reference program's by a relative error of at most 0.0001.
Values sent between devices are 32-bit elements; how exact they have to be, the bound alone decides.
A program may use at most 256 MiB of HBM per device.

```python
import jax
import jax.numpy as jnp
from jax import lax

V = 12
C = 12
AGG = 4
NX = 64
NT = 8
NZ = 16
NY = 16
NAGG = 16
N_TA = 2
N_GZ = 4
N_GY = 4


def draw_near_null(key, part):
    key_base, key_site, key_vector = jax.random.split(key, 3)
    shape = (NT, NZ, NY, V, C, 2 * NX)
    site_scale = jnp.exp(jax.random.uniform(key_site, (NT, NZ, NY, 1, 1, 2 * NX), jnp.float32) * jnp.log(10.0))
    vector_scale = jnp.exp(jax.random.uniform(key_vector, (1, 1, 1, V, 1, 1), jnp.float32) * jnp.log(10.0))
    base = jnp.clip(jax.random.normal(key_base, shape, jnp.float32), -4.0, 4.0)
    return (base * site_scale * vector_scale).astype(jnp.float32)


def with_ends(entries, rng, smallest, high):
    longest = entries.shape.index(max(entries.shape))
    spots = []
    for shift in (0, 1):
        where = [jax.random.randint(jax.random.fold_in(rng, axis), (), 0, length) for axis, length in enumerate(entries.shape)]
        where[longest] = (where[longest] + shift) % entries.shape[longest]
        spots.append(tuple(where))
    return entries.at[spots[0]].set(smallest).at[spots[1]].set(high)


def setup_inputs(seed: int = 0) -> dict:
    key_of = jax.random.split(jax.random.key(seed), 4)
    near_null = draw_near_null(jax.random.fold_in(key_of[3], 71), 0)
    offsets = with_ends(jax.random.randint(key_of[1], (4,), 1, AGG), jax.random.fold_in(key_of[1], 1), 1, AGG - 1).astype(jnp.int32)
    owner_slot = jax.vmap(lambda own: jax.random.permutation(own, NAGG))(jax.random.split(key_of[2], N_TA * N_GZ * N_GY)).reshape((N_TA, N_GZ, N_GY, NAGG)).astype(jnp.int32)
    return {"near_null": near_null, "offsets": offsets, "owner_slot": owner_slot}


ridge_scale = 0.05
top_precision = lax.Precision.HIGHEST

def factor_pass(blocks):
    norm_count = blocks.shape[3] * blocks.shape[5]
    products = jnp.einsum('nkvcas,nkwcbs->nkavbw', blocks, blocks, precision=top_precision) / norm_count
    gram_real = products[:, :, 0, :, 0, :] + products[:, :, 1, :, 1, :]
    gram_imag = products[:, :, 0, :, 1, :] - products[:, :, 1, :, 0, :]
    width = gram_real.shape[-1]
    diag_mean = lax.optimization_barrier(jnp.mean(jnp.diagonal(gram_real, axis1=2, axis2=3), axis=-1))
    ridge_term = ridge_scale * (diag_mean + 1e-06)
    gram_real = jnp.moveaxis(gram_real, (2, 3), (0, 1))
    gram_imag = jnp.moveaxis(gram_imag, (2, 3), (0, 1))
    zero_batch = jnp.zeros_like(ridge_term)
    low_real = [[zero_batch] * width for row_idx in range(width)]
    low_imag = [[zero_batch] * width for row_idx in range(width)]
    for col_idx in range(width):
        remain = gram_real[col_idx, col_idx] + ridge_term
        for mid_idx in range(col_idx):
            remain = remain - low_real[col_idx][mid_idx] * low_real[col_idx][mid_idx]
            remain = remain - low_imag[col_idx][mid_idx] * low_imag[col_idx][mid_idx]
        diag_val = jnp.sqrt(remain)
        low_real[col_idx][col_idx] = diag_val
        for row_idx in range(col_idx + 1, width):
            sum_real = gram_real[row_idx, col_idx]
            sum_imag = gram_imag[row_idx, col_idx]
            for mid_idx in range(col_idx):
                left_real = low_real[row_idx][mid_idx]
                left_imag = low_imag[row_idx][mid_idx]
                right_real = low_real[col_idx][mid_idx]
                right_imag = low_imag[col_idx][mid_idx]
                sum_real = sum_real - (left_real * right_real + left_imag * right_imag)
                sum_imag = sum_imag - (left_imag * right_real - left_real * right_imag)
            low_real[row_idx][col_idx] = sum_real / diag_val
            low_imag[row_idx][col_idx] = sum_imag / diag_val
    inv_real = [[zero_batch] * width for row_idx in range(width)]
    inv_imag = [[zero_batch] * width for row_idx in range(width)]
    for col_idx in range(width):
        inv_real[col_idx][col_idx] = 1.0 / low_real[col_idx][col_idx]
        for row_idx in range(col_idx + 1, width):
            sum_real = zero_batch
            sum_imag = zero_batch
            for mid_idx in range(col_idx, row_idx):
                left_real = low_real[row_idx][mid_idx]
                left_imag = low_imag[row_idx][mid_idx]
                right_real = inv_real[mid_idx][col_idx]
                right_imag = inv_imag[mid_idx][col_idx]
                sum_real = sum_real + left_real * right_real - left_imag * right_imag
                sum_imag = sum_imag + left_real * right_imag + left_imag * right_real
            inv_real[row_idx][col_idx] = -sum_real / low_real[row_idx][row_idx]
            inv_imag[row_idx][col_idx] = -sum_imag / low_real[row_idx][row_idx]
    map_real = jnp.stack([jnp.stack([inv_real[w_idx][v_idx] for w_idx in range(width)], axis=-1) for v_idx in range(width)], axis=-2)
    map_imag = -jnp.stack([jnp.stack([inv_imag[w_idx][v_idx] for w_idx in range(width)], axis=-1) for v_idx in range(width)], axis=-2)
    mixing = jnp.stack([jnp.stack([map_real, map_imag], axis=3), jnp.stack([-map_imag, map_real], axis=3)], axis=2)
    return jnp.einsum('nkvcas,nkavbw->nkwcbs', blocks, mixing, precision=top_precision)

def two_passes(blocks):
    return factor_pass(factor_pass(blocks))

def reference(near_null, offsets, owner_slot):
    lattice = near_null.reshape(NT, NZ, NY, V, C, 2, NX)
    lattice = jnp.roll(lattice, -offsets[0], axis=0)
    lattice = jnp.roll(lattice, -offsets[1], axis=1)
    lattice = jnp.roll(lattice, -offsets[2], axis=2)
    lattice = jnp.roll(lattice, -offsets[3], axis=6)
    half_c = C // 2
    pieces = lattice.reshape(N_TA, AGG, N_GZ, AGG, N_GY, AGG, V, 2, half_c, 2, NAGG, AGG)
    pieces = pieces.transpose(0, 2, 4, 10, 7, 6, 8, 9, 1, 3, 5, 11)
    site_count = AGG * AGG * AGG * AGG
    device_count = N_TA * N_GZ * N_GY
    flattened = pieces.reshape(device_count * NAGG, 2, V, half_c, 2, site_count)
    source_of = jnp.argsort(owner_slot, axis=-1).astype(jnp.int32)
    device_base = (jnp.arange(device_count, dtype=jnp.int32) * NAGG).reshape(N_TA, N_GZ, N_GY, 1)
    packed = jnp.take(flattened, (device_base + source_of).reshape(-1), axis=0)
    per_peer = NAGG // N_TA
    packed = packed.reshape(N_TA, N_GZ, N_GY, N_TA, per_peer, 2, V, half_c, 2, site_count)
    owned_aggs = packed.transpose(3, 1, 2, 0, 4, 5, 6, 7, 8, 9).reshape(device_count, NAGG, 2, V, half_c, 2, site_count)
    result = lax.map(two_passes, owned_aggs)
    return result.reshape(device_count * NAGG, 2, V, half_c, 2, site_count)
```

```python
import functools

import jax
import jax.numpy as jnp
from jax import lax
from jax.experimental import pallas as pl
from jax.experimental.pallas import tpu as pltpu
from jax.sharding import PartitionSpec as P

MAX_OFFSET = 3
MESH_ID = pl.DeviceIdType.MESH


def exchange_kernel(
    oz,
    oy,
    pieces,
    offset_ref,
    slot_ref,
    near_ref,
    keep_ref,
    got_ref,
    raw,
    home,
    side,
    kept,
    sent,
    other_slot,
    lane_from,
    in_sem,
    keep_sem,
    slot_sem,
    side_sem,
    home_sem,
    sent_sem,
    got_sem,
):
    edge = raw.shape[0]
    rows, lanes = home.shape[3:]
    chunk = rows // pieces
    count = edge * edge
    half = count // 2
    x_sites = lanes // 2
    me = lax.axis_index("ta")
    z_len, y_len = lax.axis_size("gz"), lax.axis_size("gy")
    z_at, y_at = lax.axis_index("gz"), lax.axis_index("gy")
    z_down, z_up = lax.rem(z_at + z_len - 1, z_len), lax.rem(z_at + 1, z_len)
    y_down, y_up = lax.rem(y_at + y_len - 1, y_len), lax.rem(y_at + 1, y_len)
    partner = {"ta": 1 - me}

    in_copies = [
        pltpu.make_async_copy(near_ref.at[t], raw.at[t], in_sem.at[t]) for t in range(edge)
    ]
    for copy in in_copies:
        copy.start()

    barrier = pltpu.get_barrier_semaphore()
    greeted = [
        {"gz": z_down},
        {"gy": y_down},
        {"gz": z_down, "gy": y_down},
        {"gz": z_up},
        {"gy": y_up},
        {"gz": z_up, "gy": y_up},
        partner,
    ]
    for target in greeted:
        pl.semaphore_signal(barrier, inc=1, device_id=target, device_id_type=MESH_ID)
    pl.semaphore_wait(barrier, len(greeted))

    slot_copy = pltpu.make_async_remote_copy(
        src_ref=slot_ref,
        dst_ref=other_slot,
        send_sem=slot_sem.at[0],
        recv_sem=slot_sem.at[1],
        device_id=partner,
        device_id_type=MESH_ID,
    )
    slot_copy.start()

    near_z, far_z = (0, edge - oz), (edge - oz, oz)
    near_y, far_y = (0, edge - oy), (edge - oy, oy)
    parts = [
        (near_z, far_y, {"gy": y_down}),
        (far_z, far_y, {"gz": z_down, "gy": y_down}),
        (far_z, near_y, {"gz": z_down}),
    ]

    def part_copies(t, r):
        at = pl.ds(pl.multiple_of(r * chunk, chunk), chunk)
        made = []
        for n, ((z0, zn), (y0, yn), target) in enumerate(parts):
            made.append(
                pltpu.make_async_remote_copy(
                    src_ref=side.at[t, pl.ds(z0, zn), pl.ds(y0, yn), at],
                    dst_ref=home.at[t, pl.ds(z0, zn), pl.ds(y0, yn), at],
                    send_sem=side_sem.at[n, t, r],
                    recv_sem=home_sem.at[n, t, r],
                    device_id=target,
                    device_id_type=MESH_ID,
                )
            )
        return made

    def sent_copy(t, r):
        at = pl.ds(pl.multiple_of(r * chunk, chunk), chunk)
        return pltpu.make_async_remote_copy(
            src_ref=sent.at[t, :, at],
            dst_ref=got_ref.at[t, :, at],
            send_sem=sent_sem.at[t, r],
            recv_sem=got_sem.at[t, r],
            device_id=partner,
            device_id_type=MESH_ID,
        )

    def keep_copy(t):
        return pltpu.make_async_copy(kept.at[t], keep_ref.at[t], keep_sem.at[t])

    def pack_piece(t, r):
        start = pl.multiple_of(r * chunk, chunk)
        for z in range(edge):
            for y in range(edge):
                target = home if z >= oz and y >= oy else side
                target[t, (z - oz) % edge, (y - oy) % edge, pl.ds(start, chunk), :] = raw[
                    t, z, pl.ds(start * edge + y, chunk, stride=edge), :
                ]

    def send_parts(t, r):
        for copy in part_copies(t, r):
            copy.start()

    def pack_row(t, carry):
        pltpu.make_async_copy(near_ref.at[t], raw.at[t], in_sem.at[t]).wait()

        def body(r, inner):
            pack_piece(t, r)
            send_parts(t, r)
            return inner

        return lax.fori_loop(0, pieces, body, carry)

    lax.fori_loop(0, edge, pack_row, 0)

    lane = lax.broadcasted_iota(jnp.int32, (8, lanes), 1)
    group = edge.bit_length() - 1
    wanted = ((lane >> group) & (count - 1)) ^ (me * half)

    def lanes_of(slots):
        found = jnp.zeros((8, lanes), jnp.int32)
        for j in range(count):
            slot = jnp.broadcast_to(slots[0:1, j : j + 1], (8, lanes))
            found = jnp.where(slot == wanted, j, found)
        x = (found * edge + (lane & (edge - 1)) + offset_ref[3]) & (x_sites - 1)
        return (lane & x_sites) + x

    lane_from[0] = lanes_of(slot_ref[...])
    slot_copy.wait()
    lane_from[1] = lanes_of(other_slot[...])

    def regroup_piece(t, r):
        start = pl.multiple_of(r * chunk, chunk)
        moved = jnp.where(t >= offset_ref[0], lane_from[0], lane_from[1])
        for g in range(chunk // 8):
            at = pl.ds(pl.multiple_of(start + g * 8, 8), 8)
            units = [
                jnp.take_along_axis(
                    home[t, u // edge, u % edge, at, :], moved, axis=1, mode="promise_in_bounds"
                )
                for u in range(count)
            ]
            bit = 1
            while bit < count:
                step = bit * edge
                high = (lane & step) != 0
                fresh = list(units)
                for u in range(count):
                    if not u & bit:
                        low_unit, high_unit = units[u], units[u + bit]
                        fresh[u] = jnp.where(high, pltpu.roll(high_unit, step, 1), low_unit)
                        fresh[u + bit] = jnp.where(
                            high, high_unit, pltpu.roll(low_unit, lanes - step, 1)
                        )
                units = fresh
                bit *= 2
            for j in range(half):
                sent[t, j, at, :] = units[half + j]
            for j in range(half):
                kept[t, j, at, :] = units[j]

    def regroup_row(t, carry):
        def body(r, inner):
            for copy in part_copies(t, r):
                copy.wait_recv()
            regroup_piece(t, r)
            sent_copy(t, r).start()
            return inner

        carry = lax.fori_loop(0, pieces, body, carry)
        keep_copy(t).start()
        return carry

    lax.fori_loop(0, edge, regroup_row, 0)

    def finish_row(t, carry):
        def body(r, inner):
            for copy in part_copies(t, r):
                copy.wait_send()
            sent_copy(t, r).wait()
            return inner

        carry = lax.fori_loop(0, pieces, body, carry)
        keep_copy(t).wait()
        return carry

    lax.fori_loop(0, edge, finish_row, 0)


def exchange(oz, oy, call_id, offsets, slots, lattice):
    edge, _, all_rows, lanes = lattice.shape
    rows = all_rows // edge
    pieces = max(p for p in range(1, 7) if rows % (8 * p) == 0)
    half = edge * edge // 2
    size = lattice.size
    out = jax.ShapeDtypeStruct((edge, half, rows, lanes), jnp.float32)
    block = (edge, half, rows, lanes)
    whole = (edge, edge, edge, rows, lanes)
    return pl.pallas_call(
        functools.partial(exchange_kernel, oz, oy, pieces),
        in_specs=[
            pl.BlockSpec(memory_space=pltpu.SMEM),
            pl.BlockSpec(memory_space=pltpu.VMEM),
            pl.BlockSpec(memory_space=pl.ANY),
        ],
        out_specs=[pl.BlockSpec(memory_space=pl.ANY)] * 2,
        out_shape=[out, out],
        scratch_shapes=[
            pltpu.VMEM(lattice.shape, jnp.float32),
            pltpu.VMEM(whole, jnp.float32),
            pltpu.VMEM(whole, jnp.float32),
            pltpu.VMEM(block, jnp.float32),
            pltpu.VMEM(block, jnp.float32),
            pltpu.VMEM(slots.shape, jnp.int32),
            pltpu.VMEM((2, 8, lanes), jnp.int32),
            pltpu.SemaphoreType.DMA((edge,)),
            pltpu.SemaphoreType.DMA((edge,)),
            pltpu.SemaphoreType.DMA((2,)),
            pltpu.SemaphoreType.DMA((3, edge, pieces)),
            pltpu.SemaphoreType.DMA((3, edge, pieces)),
            pltpu.SemaphoreType.DMA((edge, pieces)),
            pltpu.SemaphoreType.DMA((edge, pieces)),
        ],
        compiler_params=pltpu.CompilerParams(
            collective_id=call_id,
            has_side_effects=True,
            vmem_limit_bytes=40 * 1024 * 1024,
        ),
        cost_estimate=pl.CostEstimate(flops=size * 10, bytes_accessed=size * 9, transcendentals=0),
    )(offsets, slots, lattice)


def matmul_rows(left, right):
    out = []
    for v in range(len(left)):
        real = imag = None
        for m in range(v + 1):
            a = left[v][0][m : m + 1, :]
            b = left[v][1][m : m + 1, :]
            r, i = right[m]
            term_real, term_imag = a * r - b * i, a * i + b * r
            real = term_real if real is None else real + term_real
            imag = term_imag if imag is None else imag + term_imag
        out.append((real, imag))
    return out


def invert_factor(gram, width):
    row_of = lax.broadcasted_iota(jnp.int32, gram[0][0].shape, 0)
    mean = gram[0][0][0:1, :]
    for v in range(1, width):
        mean = mean + gram[v][0][v : v + 1, :]
    ridge = 0.05 * (mean / width + 1e-06)
    rows = [(jnp.where(row_of == v, r + ridge, r), i) for v, (r, i) in enumerate(gram)]
    zero = jnp.zeros_like(rows[0][0])
    inverse = [(jnp.where(row_of == v, 1.0, zero), zero) for v in range(width)]
    for k in range(width):
        scale = 1.0 / jnp.sqrt(rows[k][0][k : k + 1, :])
        pivot = (rows[k][0] * scale, rows[k][1] * scale)
        known = (inverse[k][0] * scale, inverse[k][1] * scale)
        inverse[k] = known
        for v in range(k + 1, width):
            a = pivot[0][v : v + 1, :]
            b = -pivot[1][v : v + 1, :]
            r, i = rows[v]
            rows[v] = (r - (a * pivot[0] - b * pivot[1]), i - (a * pivot[1] + b * pivot[0]))
            r, i = inverse[v]
            inverse[v] = (r - (a * known[0] - b * known[1]), i - (a * known[1] + b * known[0]))
    return inverse


def split(x):
    high = x.astype(jnp.bfloat16)
    return high, (x - high.astype(jnp.float32)).astype(jnp.bfloat16)


def factor_kernel(
    vectors,
    offset_ref,
    keep_ref,
    got_ref,
    out_ref,
    tiles,
    parted,
    stage,
    gram,
    turn,
    in_sem,
    out_sem,
):
    _, per_home, edge, unit_rows, lanes = tiles.shape
    comps = unit_rows // vectors
    kinds = comps // 2
    count = 2 * per_home
    batch = 2 * count
    padded = 16
    pitch = gram.shape[0] // batch
    mid = lanes // 2
    norm = 1.0 / (kinds * edge**4)
    me = lax.axis_index("ta")
    ot = offset_ref[0]

    def in_copies(t):
        place = jnp.where(t >= ot, me, 1 - me)
        row = (t - ot) & (edge - 1)
        return [
            pltpu.make_async_copy(keep_ref.at[t], tiles.at[place, :, row], in_sem.at[0, t]),
            pltpu.make_async_copy(got_ref.at[t], tiles.at[1 - place, :, row], in_sem.at[1, t]),
        ]

    for t in range(edge):
        for copy in in_copies(t):
            copy.start()
    for t in range(edge):
        for copy in in_copies(t):
            copy.wait()
    zeros = jnp.zeros((padded - vectors, lanes), jnp.float32)
    low = lax.broadcasted_iota(jnp.int32, (padded, lanes), 1) < mid

    def gram_of(n, carry):
        at_home, slot = n // per_home, n % per_home
        for h in range(2):
            b = n * 2 + h
            for k in range(kinds):
                for s in range(edge // 2):
                    one, two = (
                        jnp.concatenate(
                            [
                                tiles[
                                    at_home,
                                    slot,
                                    2 * s + w,
                                    pl.ds(h * kinds + k, vectors, stride=comps),
                                    :,
                                ],
                                zeros,
                            ],
                            axis=0,
                        )
                        for w in range(2)
                    )
                    real = jnp.where(low, one, pltpu.roll(two, mid, 1))
                    imag = jnp.where(low, pltpu.roll(one, mid, 1), two)
                    at = (k * (edge // 2) + s) * lanes
                    for w, value in enumerate(split(real) + split(imag)):
                        row = (w % 2) * 2 + w // 2
                        parted[b, row * padded : (row + 1) * padded, at : at + lanes] = value
            both = parted[b]
            products = lax.dot_general(
                both,
                both,
                (((1,), (1,)), ((), ())),
                preferred_element_type=jnp.float32,
            )
            start = pl.multiple_of(b * pitch, 8)
            gram[pl.ds(start, 2 * padded), 0 : 4 * padded] = (
                products[: 2 * padded] + products[2 * padded :]
            ) * norm
        return carry

    lax.fori_loop(0, count, gram_of, 0)

    first = []
    for v in range(vectors):
        top = gram[pl.ds(v, batch, stride=pitch), :].T
        low_part = gram[pl.ds(padded + v, batch, stride=pitch), :].T
        top = top[: 2 * padded] + top[2 * padded : 4 * padded]
        low_part = low_part[: 2 * padded] + low_part[2 * padded : 4 * padded]
        first.append((top[:padded] + low_part[padded:], top[padded:] - low_part[:padded]))
    inverse = invert_factor(first, vectors)
    moved = matmul_rows(inverse, first)
    for v in range(padded):
        for w in range(2):
            turn[w, v * padded : (v + 1) * padded, :] = (
                moved[v][w] if v < vectors else jnp.zeros((padded, batch), jnp.float32)
            )
    flipped = [
        (turn[0, pl.ds(m, padded, stride=padded), :], -turn[1, pl.ds(m, padded, stride=padded), :])
        for m in range(vectors)
    ]
    second = matmul_rows(inverse, flipped)
    final = matmul_rows(invert_factor(second, vectors), inverse)
    rest = jnp.zeros((lanes - 3 * padded, batch), jnp.float32)
    for w in range(vectors):
        block = jnp.concatenate([final[w][0], final[w][1], -final[w][0], rest], axis=0)
        gram[pl.ds(w, batch, stride=pitch), :] = block.T
    for w in range(vectors, padded):
        gram[pl.ds(w, batch, stride=pitch), :] = jnp.zeros((batch, lanes), jnp.float32)

    def out_copy(n, slot):
        return pltpu.make_async_copy(stage.at[slot], out_ref.at[n], out_sem.at[slot])

    def apply_to(n, carry):
        slot = n % 2

        @pl.when(n >= 2)
        def _():
            out_copy(n - 2, slot).wait()

        for h in range(2):
            b = n * 2 + h
            start = pl.multiple_of(b * pitch, 8)
            mixing = gram[pl.ds(start, padded), :]
            plain, minus = mixing[:, : 2 * padded], -mixing[:, padded : 3 * padded]
            full_high, full_low = split(jnp.concatenate([plain, minus], axis=0))
            left = jnp.concatenate(
                [
                    jnp.concatenate([full_high, full_high], axis=1),
                    jnp.concatenate([full_low, jnp.zeros_like(full_low)], axis=1),
                ],
                axis=0,
            )
            made = jnp.dot(left, parted[b], preferred_element_type=jnp.float32)
            made = made[: 2 * padded] + made[2 * padded :]
            for k in range(kinds):
                for s in range(edge // 2):
                    at = (k * (edge // 2) + s) * lanes
                    row = k * edge + 2 * s
                    stride = kinds * edge
                    for w in range(2):
                        stage[slot, h, pl.ds(row + w, vectors, stride=stride), :] = made[
                            w * padded : w * padded + vectors, at : at + lanes
                        ]
        out_copy(n, slot).start()
        return carry

    lax.fori_loop(0, count, apply_to, 0)
    out_copy(count - 2, 0).wait()
    out_copy(count - 1, 1).wait()


def factor(vectors, offsets, keep, got):
    edge, per_home, unit_rows, lanes = keep.shape
    comps = unit_rows // vectors
    count = 2 * per_home
    batch = 2 * count
    pitch = 40
    out_rows = vectors * comps // 2 * edge
    size = count * edge * unit_rows * lanes
    return pl.pallas_call(
        functools.partial(factor_kernel, vectors),
        in_specs=[pl.BlockSpec(memory_space=pltpu.SMEM)]
        + [pl.BlockSpec(memory_space=pl.ANY)] * 2,
        out_specs=pl.BlockSpec(memory_space=pl.ANY),
        out_shape=jax.ShapeDtypeStruct((count, 2, out_rows, lanes), jnp.float32),
        scratch_shapes=[
            pltpu.VMEM((2, per_home, edge, unit_rows, lanes), jnp.float32),
            pltpu.VMEM((batch, 64, comps // 2 * (edge // 2) * lanes), jnp.bfloat16),
            pltpu.VMEM((2, 2, out_rows, lanes), jnp.float32),
            pltpu.VMEM((batch * pitch, lanes), jnp.float32),
            pltpu.VMEM((2, 16 * 16, batch), jnp.float32),
            pltpu.SemaphoreType.DMA((2, edge)),
            pltpu.SemaphoreType.DMA((2,)),
        ],
        compiler_params=pltpu.CompilerParams(vmem_limit_bytes=48 * 1024 * 1024),
        cost_estimate=pl.CostEstimate(flops=size * 100, bytes_accessed=size * 8, transcendentals=0),
    )(offsets, keep, got)


def per_device_pair(near_null, offsets, owner_slot):
    edge = near_null.shape[0]
    vectors, comps = near_null.shape[3:5]
    slots = owner_slot.reshape(1, -1)
    lattice = near_null.transpose(0, 1, 3, 4, 2, 5).reshape(
        edge, near_null.shape[1], -1, near_null.shape[5]
    )
    branches = [
        functools.partial(exchange, oz, oy, (oz - 1) * MAX_OFFSET + oy - 1)
        for oz in range(1, MAX_OFFSET + 1)
        for oy in range(1, MAX_OFFSET + 1)
    ]
    which = (offsets[1] - 1) * MAX_OFFSET + offsets[2] - 1
    keep, got = lax.switch(which, branches, offsets, slots, lattice)
    made = factor(vectors, offsets, keep, got)
    count = made.shape[0]
    kinds = comps // 2
    made = made.reshape(count, 2, vectors, kinds, edge // 2, 2, made.shape[-1])
    return made.transpose(0, 1, 2, 3, 5, 4, 6).reshape(
        count, 2, vectors, kinds, 2, edge // 2 * made.shape[-1]
    )


ridge_scale = 0.05
top_precision = lax.Precision.HIGHEST


def from_behind(array, axis, by):
    length = lax.axis_size(axis)
    return lax.ppermute(array, axis, [(i, (i + by) % length) for i in range(length)])


def factor_pass(blocks):
    norm_count = blocks.shape[3] * blocks.shape[5]
    products = (
        jnp.einsum("nkvcas,nkwcbs->nkavbw", blocks, blocks, precision=top_precision) / norm_count
    )
    gram_real = products[:, :, 0, :, 0, :] + products[:, :, 1, :, 1, :]
    gram_imag = products[:, :, 0, :, 1, :] - products[:, :, 1, :, 0, :]
    width = gram_real.shape[-1]
    diag_mean = jnp.mean(jnp.diagonal(gram_real, axis1=2, axis2=3), axis=-1)
    ridge_term = ridge_scale * (diag_mean + 1e-06)
    gram_real = jnp.moveaxis(gram_real, (2, 3), (0, 1))
    gram_imag = jnp.moveaxis(gram_imag, (2, 3), (0, 1))
    zero_batch = jnp.zeros_like(ridge_term)
    low_real = [[zero_batch] * width for row_idx in range(width)]
    low_imag = [[zero_batch] * width for row_idx in range(width)]
    for col_idx in range(width):
        remain = gram_real[col_idx, col_idx] + ridge_term
        for mid_idx in range(col_idx):
            remain = remain - low_real[col_idx][mid_idx] * low_real[col_idx][mid_idx]
            remain = remain - low_imag[col_idx][mid_idx] * low_imag[col_idx][mid_idx]
        diag_val = jnp.sqrt(remain)
        low_real[col_idx][col_idx] = diag_val
        for row_idx in range(col_idx + 1, width):
            sum_real = gram_real[row_idx, col_idx]
            sum_imag = gram_imag[row_idx, col_idx]
            for mid_idx in range(col_idx):
                left_real = low_real[row_idx][mid_idx]
                left_imag = low_imag[row_idx][mid_idx]
                right_real = low_real[col_idx][mid_idx]
                right_imag = low_imag[col_idx][mid_idx]
                sum_real = sum_real - (left_real * right_real + left_imag * right_imag)
                sum_imag = sum_imag - (left_imag * right_real - left_real * right_imag)
            low_real[row_idx][col_idx] = sum_real / diag_val
            low_imag[row_idx][col_idx] = sum_imag / diag_val
    inv_real = [[zero_batch] * width for row_idx in range(width)]
    inv_imag = [[zero_batch] * width for row_idx in range(width)]
    for col_idx in range(width):
        inv_real[col_idx][col_idx] = 1.0 / low_real[col_idx][col_idx]
        for row_idx in range(col_idx + 1, width):
            sum_real = zero_batch
            sum_imag = zero_batch
            for mid_idx in range(col_idx, row_idx):
                left_real = low_real[row_idx][mid_idx]
                left_imag = low_imag[row_idx][mid_idx]
                right_real = inv_real[mid_idx][col_idx]
                right_imag = inv_imag[mid_idx][col_idx]
                sum_real = sum_real + left_real * right_real - left_imag * right_imag
                sum_imag = sum_imag + left_real * right_imag + left_imag * right_real
            inv_real[row_idx][col_idx] = -sum_real / low_real[row_idx][row_idx]
            inv_imag[row_idx][col_idx] = -sum_imag / low_real[row_idx][row_idx]
    map_real = jnp.stack(
        [
            jnp.stack([inv_real[w_idx][v_idx] for w_idx in range(width)], axis=-1)
            for v_idx in range(width)
        ],
        axis=-2,
    )
    map_imag = -jnp.stack(
        [
            jnp.stack([inv_imag[w_idx][v_idx] for w_idx in range(width)], axis=-1)
            for v_idx in range(width)
        ],
        axis=-2,
    )
    mixing = jnp.stack(
        [jnp.stack([map_real, map_imag], axis=3), jnp.stack([-map_imag, map_real], axis=3)], axis=2
    )
    return jnp.einsum("nkvcas,nkavbw->nkwcbs", blocks, mixing, precision=top_precision)


def two_passes(blocks):
    return factor_pass(factor_pass(blocks))


def arrange(lattice, row_count, agg_edge):
    vector_count = lattice.shape[3]
    comp_count = lattice.shape[4]
    x_sites = lattice.shape[6]
    groups = x_sites // agg_edge
    pieces = lattice.reshape(
        row_count, agg_edge, agg_edge, vector_count, 2, comp_count // 2, 2, groups, agg_edge
    )
    pieces = pieces.transpose(7, 4, 3, 5, 6, 0, 1, 2, 8)
    return pieces.reshape(
        groups, 2, vector_count, comp_count // 2, 2, row_count * agg_edge * agg_edge * agg_edge
    )


def invert(slot_row):
    places = jnp.arange(slot_row.shape[0], dtype=jnp.int32)
    return jnp.sum(jnp.where(slot_row[None, :] == places[:, None], places[None, :], 0), axis=1)


def per_device_general(near_null, offsets, owner_slot):
    agg_edge = near_null.shape[0]
    rim_rows = agg_edge - 1
    from_z = from_behind(near_null[:, :rim_rows], "gz", -1)
    lattice = lax.dynamic_slice_in_dim(
        jnp.concatenate([near_null, from_z], axis=1), offsets[1], agg_edge, 1
    )
    from_y = from_behind(lattice[:, :, :rim_rows], "gy", -1)
    lattice = lax.dynamic_slice_in_dim(
        jnp.concatenate([lattice, from_y], axis=2), offsets[2], agg_edge, 2
    )
    x_sites = lattice.shape[5] // 2
    lattice = lattice.reshape(lattice.shape[:5] + (2, x_sites))
    lattice = lax.dynamic_slice_in_dim(
        jnp.concatenate([lattice, lattice], axis=6), offsets[3], x_sites, 6
    )
    slot_row = owner_slot.reshape(-1)
    source_of = invert(slot_row)
    from_t = from_behind(lattice[:rim_rows], "ta", -1)
    lattice = lax.dynamic_slice_in_dim(
        jnp.concatenate([lattice, from_t], axis=0), offsets[0], agg_edge, 0
    )
    tiles = arrange(lattice, agg_edge, agg_edge)
    packed = jnp.take(tiles, source_of, axis=0)
    result = two_passes(lax.all_to_all(packed, "ta", split_axis=0, concat_axis=0, tiled=True))
    return result


def solution(mesh):
    pair = mesh.shape["ta"] == 2 and mesh.shape["gz"] > 1 and mesh.shape["gy"] > 1
    return jax.shard_map(
        per_device_pair if pair else per_device_general,
        mesh=mesh,
        in_specs=(P("ta", "gz", "gy", None, None, None), P(), P("ta", "gz", "gy", None)),
        out_specs=P(("ta", "gz", "gy"), None, None, None, None, None),
        check_vma=False,
    )
```

```python
import functools

import jax
import jax.numpy as jnp
from jax import lax
from jax.experimental import pallas as pl
from jax.experimental.pallas import tpu as pltpu
from jax.sharding import PartitionSpec as P

MAX_OFFSET = 3
LEAD = 4
GRAM_PITCH = 24
MIX_PITCH = 40
MESH_ID = pl.DeviceIdType.MESH


def split(x):
    high = x.astype(jnp.bfloat16)
    return high, (x - high.astype(jnp.float32)).astype(jnp.bfloat16)


def exchange_kernel(
    oz,
    oy,
    pieces,
    vectors,
    offset_ref,
    slot_ref,
    near_ref,
    owned,
    total,
    raw,
    home,
    side,
    sent,
    other_slot,
    lane_from,
    in_sem,
    slot_sem,
    side_sem,
    home_sem,
    sent_sem,
    got_sem,
):
    edge = raw.shape[0]
    rows, lanes = home.shape[3:]
    chunk = rows // pieces
    count = edge * edge
    half = count // 2
    x_sites = lanes // 2
    me = lax.axis_index("ta")
    z_len, y_len = lax.axis_size("gz"), lax.axis_size("gy")
    z_at, y_at = lax.axis_index("gz"), lax.axis_index("gy")
    z_down, z_up = lax.rem(z_at + z_len - 1, z_len), lax.rem(z_at + 1, z_len)
    y_down, y_up = lax.rem(y_at + y_len - 1, y_len), lax.rem(y_at + 1, y_len)
    partner = {"ta": 1 - me}

    def in_copy(t, r):
        at = pl.ds(pl.multiple_of(r * chunk * edge, chunk * edge), chunk * edge)
        return pltpu.make_async_copy(near_ref.at[t, :, at], raw.at[t, :, at], in_sem.at[t, r])

    def start_in(i, carry):
        in_copy(i // pieces, i % pieces).start()
        return carry

    lax.fori_loop(0, edge * pieces, start_in, 0)

    barrier = pltpu.get_barrier_semaphore()
    greeted = [
        {"gz": z_down},
        {"gy": y_down},
        {"gz": z_down, "gy": y_down},
        {"gz": z_up},
        {"gy": y_up},
        {"gz": z_up, "gy": y_up},
        partner,
    ]
    for target in greeted:
        pl.semaphore_signal(barrier, inc=1, device_id=target, device_id_type=MESH_ID)
    pl.semaphore_wait(barrier, len(greeted))

    slot_copy = pltpu.make_async_remote_copy(
        src_ref=slot_ref,
        dst_ref=other_slot,
        send_sem=slot_sem.at[0],
        recv_sem=slot_sem.at[1],
        device_id=partner,
        device_id_type=MESH_ID,
    )
    slot_copy.start()

    near_z, far_z = (0, edge - oz), (edge - oz, oz)
    near_y, far_y = (0, edge - oy), (edge - oy, oy)
    parts = [
        (near_z, far_y, {"gy": y_down}),
        (far_z, far_y, {"gz": z_down, "gy": y_down}),
        (far_z, near_y, {"gz": z_down}),
    ]

    def part_copies(t, r):
        at = pl.ds(pl.multiple_of(r * chunk, chunk), chunk)
        made = []
        for n, ((z0, zn), (y0, yn), target) in enumerate(parts):
            made.append(
                pltpu.make_async_remote_copy(
                    src_ref=side.at[t, pl.ds(z0, zn), pl.ds(y0, yn), at],
                    dst_ref=home.at[t, pl.ds(z0, zn), pl.ds(y0, yn), at],
                    send_sem=side_sem.at[n, t, r],
                    recv_sem=home_sem.at[n, t, r],
                    device_id=target,
                    device_id_type=MESH_ID,
                )
            )
        return made

    def sent_copy(t, r):
        at = pl.ds(pl.multiple_of(r * chunk, chunk), chunk)
        return pltpu.make_async_remote_copy(
            src_ref=sent.at[t, :, at],
            dst_ref=owned.at[1, t, :, at],
            send_sem=sent_sem.at[t, r],
            recv_sem=got_sem.at[t, r],
            device_id=partner,
            device_id_type=MESH_ID,
        )

    def pack_piece(t, r):
        start = pl.multiple_of(r * chunk, chunk)
        for z in range(edge):
            for y in range(edge):
                target = home if z >= oz and y >= oy else side
                target[t, (z - oz) % edge, (y - oy) % edge, pl.ds(start, chunk), :] = raw[
                    t, z, pl.ds(start * edge + y, chunk, stride=edge), :
                ]

    def send_parts(t, r):
        for copy in part_copies(t, r):
            copy.start()

    def pack_next(i):
        t, r = i // pieces, i % pieces
        in_copy(t, r).wait()
        pack_piece(t, r)
        send_parts(t, r)

    def pack_first(i, carry):
        pack_next(i)
        return carry

    lead = min(LEAD, edge * pieces)
    lax.fori_loop(0, lead, pack_first, 0)
    total[...] = jnp.zeros_like(total)

    lane = lax.broadcasted_iota(jnp.int32, (8, lanes), 1)
    group = edge.bit_length() - 1
    wanted = ((lane >> group) & (count - 1)) ^ (me * half)

    def lanes_of(slots):
        found = jnp.zeros((8, lanes), jnp.int32)
        for j in range(count):
            slot = jnp.broadcast_to(slots[0:1, j : j + 1], (8, lanes))
            found = jnp.where(slot == wanted, j, found)
        x = (found * edge + (lane & (edge - 1)) + offset_ref[3]) & (x_sites - 1)
        return (lane & x_sites) + x

    lane_from[0] = lanes_of(slot_ref[...])
    slot_copy.wait()
    lane_from[1] = lanes_of(other_slot[...])

    def regroup_piece(t, r):
        start = pl.multiple_of(r * chunk, chunk)
        moved = jnp.where(t >= offset_ref[0], lane_from[0], lane_from[1])
        for g in range(chunk // 8):
            at = pl.ds(pl.multiple_of(start + g * 8, 8), 8)
            units = [
                jnp.take_along_axis(
                    home[t, u // edge, u % edge, at, :], moved, axis=1, mode="promise_in_bounds"
                )
                for u in range(count)
            ]
            bit = 1
            while bit < count:
                step = bit * edge
                high = (lane & step) != 0
                fresh = list(units)
                for u in range(count):
                    if not u & bit:
                        low_unit, high_unit = units[u], units[u + bit]
                        fresh[u] = jnp.where(high, pltpu.roll(high_unit, step, 1), low_unit)
                        fresh[u + bit] = jnp.where(
                            high, high_unit, pltpu.roll(low_unit, lanes - step, 1)
                        )
                units = fresh
                bit *= 2
            for j in range(half):
                sent[t, j, at, :] = units[half + j]
            for j in range(half):
                owned[0, t, j, at, :] = units[j]

    comps = rows // vectors
    kinds = comps // 2
    padded = 16
    pitch = total.shape[0] // (4 * half)
    low = lax.broadcasted_iota(jnp.int32, (padded, lanes), 1) < x_sites
    zeros = jnp.zeros((padded - vectors, lanes), jnp.float32)

    def gram_row(source, t, ours):
        def gram_of(q, h):
            values = [[], [], [], []]
            for k in range(kinds):
                piece = owned[source, t, q, pl.ds(h * kinds + k, vectors, stride=comps), :]
                piece = jnp.concatenate([piece, zeros], axis=0)
                turned = pltpu.roll(piece, x_sites, 1)
                turned = jnp.where(low, turned, -turned)
                for n, value in enumerate(split(piece) + split(turned)):
                    values[n].append(value)
            both = jnp.concatenate([jnp.concatenate(v, axis=1) for v in values], axis=0)
            products = lax.dot_general(
                both[: 2 * padded],
                both,
                (((1,), (1,)), ((), ())),
                preferred_element_type=jnp.float32,
            )
            products = products[:padded] + products[padded:]
            for side_of, value in enumerate(
                (jnp.where(ours, products, 0.0), jnp.where(ours, 0.0, products))
            ):
                start = ((side_of * half + q) * 2 + h) * pitch
                at = pl.ds(pl.multiple_of(start, 8), padded)
                total[at, : 4 * padded] += value

        def body(i, carry):
            for q in range(2):
                for h in range(2):
                    gram_of(i * 2 + q, h)
            return carry

        lax.fori_loop(0, half // 2, body, 0)

    def take_got(t):
        def body(r, carry):
            sent_copy(t, r).wait_recv()
            return carry

        lax.fori_loop(0, pieces, body, 0)
        gram_row(1, t, t < offset_ref[0])

    def regroup_row(t, carry):
        def body(r, inner):
            @pl.when(t * pieces + r + lead < edge * pieces)
            def _():
                pack_next(t * pieces + r + lead)

            for copy in part_copies(t, r):
                copy.wait_recv()
            regroup_piece(t, r)
            sent_copy(t, r).start()
            return inner

        lax.fori_loop(0, pieces, body, 0)
        gram_row(0, t, t >= offset_ref[0])

        @pl.when(t >= 1)
        def _():
            take_got(t - 1)

        return carry

    lax.fori_loop(0, edge, regroup_row, 0)
    take_got(edge - 1)

    def finish_row(t, carry):
        def body(r, inner):
            for copy in part_copies(t, r):
                copy.wait_send()
            sent_copy(t, r).wait_send()
            return inner

        return lax.fori_loop(0, pieces, body, carry)

    lax.fori_loop(0, edge, finish_row, 0)


def exchange(oz, oy, call_id, vectors, offsets, slots, lattice):
    edge, _, all_rows, lanes = lattice.shape
    rows = all_rows // edge
    pieces = max(p for p in range(1, 7) if rows % (8 * p) == 0)
    half = edge * edge // 2
    size = lattice.size
    block = (edge, half, rows, lanes)
    whole = (edge, edge, edge, rows, lanes)
    sums = (4 * half * GRAM_PITCH, lanes)
    return pl.pallas_call(
        functools.partial(exchange_kernel, oz, oy, pieces, vectors),
        in_specs=[
            pl.BlockSpec(memory_space=pltpu.SMEM),
            pl.BlockSpec(memory_space=pltpu.VMEM),
            pl.BlockSpec(memory_space=pl.ANY),
        ],
        out_specs=[pl.BlockSpec(memory_space=pltpu.VMEM)] * 2,
        out_shape=[pltpu.VMEM((2,) + block, jnp.float32), pltpu.VMEM(sums, jnp.float32)],
        scratch_shapes=[
            pltpu.VMEM(lattice.shape, jnp.float32),
            pltpu.VMEM(whole, jnp.float32),
            pltpu.VMEM(whole, jnp.float32),
            pltpu.VMEM(block, jnp.float32),
            pltpu.VMEM(slots.shape, jnp.int32),
            pltpu.VMEM((2, 8, lanes), jnp.int32),
            pltpu.SemaphoreType.DMA((edge, pieces)),
            pltpu.SemaphoreType.DMA((2,)),
            pltpu.SemaphoreType.DMA((3, edge, pieces)),
            pltpu.SemaphoreType.DMA((3, edge, pieces)),
            pltpu.SemaphoreType.DMA((edge, pieces)),
            pltpu.SemaphoreType.DMA((edge, pieces)),
        ],
        compiler_params=pltpu.CompilerParams(
            collective_id=call_id,
            has_side_effects=True,
            vmem_limit_bytes=20 * 1024 * 1024,
        ),
        cost_estimate=pl.CostEstimate(flops=size * 10, bytes_accessed=size * 9, transcendentals=0),
    )(offsets, slots, lattice)


def matmul_rows(left, right):
    out = []
    for v in range(len(left)):
        real = imag = None
        for m in range(v + 1):
            a = left[v][0][m : m + 1, :]
            b = left[v][1][m : m + 1, :]
            r, i = right[m]
            term_real, term_imag = a * r - b * i, a * i + b * r
            real = term_real if real is None else real + term_real
            imag = term_imag if imag is None else imag + term_imag
        out.append((real, imag))
    return out


def invert_factor(gram, width):
    row_of = lax.broadcasted_iota(jnp.int32, gram[0][0].shape, 0)
    mean = gram[0][0][0:1, :]
    for v in range(1, width):
        mean = mean + gram[v][0][v : v + 1, :]
    ridge = 0.05 * (mean / width + 1e-06)
    rows = [(jnp.where(row_of == v, r + ridge, r), i) for v, (r, i) in enumerate(gram)]
    zero = jnp.zeros_like(rows[0][0])
    inverse = [(jnp.where(row_of == v, 1.0, zero), zero) for v in range(width)]
    for k in range(width):
        scale = 1.0 / jnp.sqrt(rows[k][0][k : k + 1, :])
        pivot = (rows[k][0] * scale, rows[k][1] * scale)
        known = (inverse[k][0] * scale, inverse[k][1] * scale)
        inverse[k] = known
        for v in range(k + 1, width):
            a = pivot[0][v : v + 1, :]
            b = -pivot[1][v : v + 1, :]
            r, i = rows[v]
            rows[v] = (r - (a * pivot[0] - b * pivot[1]), i - (a * pivot[1] + b * pivot[0]))
            r, i = inverse[v]
            inverse[v] = (r - (a * known[0] - b * known[1]), i - (a * known[1] + b * known[0]))
    return inverse


def factor_kernel(
    vectors,
    offset_ref,
    owned,
    gram,
    out_ref,
    stage,
    mix,
    turn,
    out_sem,
):
    _, edge, per_home, unit_rows, lanes = owned.shape
    comps = unit_rows // vectors
    kinds = comps // 2
    count = 2 * per_home
    batch = 2 * count
    padded = 16
    mid = lanes // 2
    norm = 1.0 / (kinds * edge**4)
    me = lax.axis_index("ta")
    ot = offset_ref[0]

    first = []
    for v in range(vectors):
        block = gram[pl.ds(v, batch, stride=GRAM_PITCH), :].T * norm
        first.append(
            (
                block[:padded] + block[padded : 2 * padded],
                block[2 * padded : 3 * padded] + block[3 * padded : 4 * padded],
            )
        )
    inverse = invert_factor(first, vectors)
    moved = matmul_rows(inverse, first)
    for v in range(padded):
        for w in range(2):
            turn[w, v * padded : (v + 1) * padded, :] = (
                moved[v][w] if v < vectors else jnp.zeros((padded, batch), jnp.float32)
            )
    flipped = [
        (turn[0, pl.ds(m, padded, stride=padded), :], -turn[1, pl.ds(m, padded, stride=padded), :])
        for m in range(vectors)
    ]
    second = matmul_rows(inverse, flipped)
    final = matmul_rows(invert_factor(second, vectors), inverse)
    rest = jnp.zeros((lanes - 6 * padded, batch), jnp.float32)
    for w in range(padded):
        if w < vectors:
            real, imag = final[w]
            blocks = ([real, imag] * 3 + [rest], [-imag, real] * 3 + [rest])
            for n, block in enumerate(blocks):
                at = pl.ds(n * padded + w, batch, stride=MIX_PITCH)
                mix[at, :] = jnp.concatenate(block, axis=0).T
        else:
            for n in range(2):
                at = pl.ds(n * padded + w, batch, stride=MIX_PITCH)
                mix[at, :] = jnp.zeros((batch, lanes), jnp.float32)

    zeros = jnp.zeros((padded - vectors, lanes), jnp.float32)
    low = lax.broadcasted_iota(jnp.int32, (padded, lanes), 1) < mid

    def out_copy(n):
        at = (me ^ (n // per_home)) * per_home + n % per_home
        return pltpu.make_async_copy(stage.at[n], out_ref.at[at], out_sem.at[n])

    is_high = lax.broadcasted_iota(jnp.int32, (2 * padded, lanes), 1) < 4 * padded

    def apply_to(n, carry):
        at_home, slot = n // per_home, n % per_home
        rows_t = [(t + ot) & (edge - 1) for t in range(edge)]
        sources = [jnp.where(t >= ot, at_home, 1 - at_home) for t in rows_t]
        for h in range(2):
            start = pl.multiple_of((n * 2 + h) * MIX_PITCH, 8)
            mixing = mix[pl.ds(start, 2 * padded), :]
            high = mixing.astype(jnp.bfloat16).astype(jnp.float32)
            left = jnp.where(is_high, high, mixing - high).astype(jnp.bfloat16)[:, : 6 * padded]
            for k in range(kinds):
                right = []
                for s in range(edge // 2):
                    one, two = (
                        jnp.concatenate(
                            [
                                owned[
                                    sources[2 * s + w],
                                    rows_t[2 * s + w],
                                    slot,
                                    pl.ds(h * kinds + k, vectors, stride=comps),
                                    :,
                                ],
                                zeros,
                            ],
                            axis=0,
                        )
                        for w in range(2)
                    )
                    real_high, real_low = split(jnp.where(low, one, pltpu.roll(two, mid, 1)))
                    imag_high, imag_low = split(jnp.where(low, pltpu.roll(one, mid, 1), two))
                    right.append(
                        jnp.concatenate(
                            [real_high, imag_high, real_low, imag_low, real_high, imag_high], axis=0
                        )
                    )
                made = jnp.dot(
                    left, jnp.concatenate(right, axis=1), preferred_element_type=jnp.float32
                )
                for s in range(edge // 2):
                    for w in range(2):
                        at = pl.ds(k * edge + 2 * s + w, vectors, stride=kinds * edge)
                        stage[n, h, at, :] = made[
                            w * padded : w * padded + vectors, s * lanes : (s + 1) * lanes
                        ]
        out_copy(n).start()
        return carry

    lax.fori_loop(0, count, apply_to, 0)

    def finish(n, carry):
        out_copy(n).wait()
        return carry

    lax.fori_loop(0, count, finish, 0)


def factor(vectors, offsets, owned, gram):
    _, edge, per_home, unit_rows, lanes = owned.shape
    comps = unit_rows // vectors
    count = 2 * per_home
    batch = 2 * count
    out_rows = vectors * comps // 2 * edge
    size = count * edge * unit_rows * lanes
    return pl.pallas_call(
        functools.partial(factor_kernel, vectors),
        in_specs=[pl.BlockSpec(memory_space=pltpu.SMEM)]
        + [pl.BlockSpec(memory_space=pltpu.VMEM)] * 2,
        out_specs=pl.BlockSpec(memory_space=pl.ANY),
        out_shape=jax.ShapeDtypeStruct((count, 2, out_rows, lanes), jnp.float32),
        scratch_shapes=[
            pltpu.VMEM((count, 2, out_rows, lanes), jnp.float32),
            pltpu.VMEM((batch * MIX_PITCH, lanes), jnp.float32),
            pltpu.VMEM((2, 16 * 16, batch), jnp.float32),
            pltpu.SemaphoreType.DMA((count,)),
        ],
        compiler_params=pltpu.CompilerParams(vmem_limit_bytes=56 * 1024 * 1024),
        cost_estimate=pl.CostEstimate(flops=size * 100, bytes_accessed=size * 8, transcendentals=0),
    )(
        offsets,
        pltpu.with_memory_space_constraint(owned, pltpu.VMEM),
        pltpu.with_memory_space_constraint(gram, pltpu.VMEM),
    )


def per_device_pair(near_null, offsets, owner_slot):
    edge = near_null.shape[0]
    vectors, comps = near_null.shape[3:5]
    slots = owner_slot.reshape(1, -1)
    lattice = near_null.transpose(0, 1, 3, 4, 2, 5).reshape(
        edge, near_null.shape[1], -1, near_null.shape[5]
    )
    def both(oz, oy, offsets, slots, lattice):
        call_id = (oz - 1) * MAX_OFFSET + oy - 1
        owned, gram = exchange(oz, oy, call_id, vectors, offsets, slots, lattice)
        made = factor(vectors, offsets, owned, gram)
        count, _, _, lanes = made.shape
        made = made.reshape(count, 2, vectors, comps // 2, edge // 2, 2, lanes)
        return made.transpose(0, 1, 2, 3, 5, 4, 6).reshape(
            count, 2, vectors, comps // 2, 2, edge // 2 * lanes
        )

    branches = [
        functools.partial(both, oz, oy)
        for oz in range(1, MAX_OFFSET + 1)
        for oy in range(1, MAX_OFFSET + 1)
    ]
    which = (offsets[1] - 1) * MAX_OFFSET + offsets[2] - 1
    return lax.switch(which, branches, offsets, slots, lattice)


ridge_scale = 0.05
top_precision = lax.Precision.HIGHEST


def from_behind(array, axis, by):
    length = lax.axis_size(axis)
    return lax.ppermute(array, axis, [(i, (i + by) % length) for i in range(length)])


def factor_pass(blocks):
    norm_count = blocks.shape[3] * blocks.shape[5]
    products = (
        jnp.einsum("nkvcas,nkwcbs->nkavbw", blocks, blocks, precision=top_precision) / norm_count
    )
    gram_real = products[:, :, 0, :, 0, :] + products[:, :, 1, :, 1, :]
    gram_imag = products[:, :, 0, :, 1, :] - products[:, :, 1, :, 0, :]
    width = gram_real.shape[-1]
    diag_mean = jnp.mean(jnp.diagonal(gram_real, axis1=2, axis2=3), axis=-1)
    ridge_term = ridge_scale * (diag_mean + 1e-06)
    gram_real = jnp.moveaxis(gram_real, (2, 3), (0, 1))
    gram_imag = jnp.moveaxis(gram_imag, (2, 3), (0, 1))
    zero_batch = jnp.zeros_like(ridge_term)
    low_real = [[zero_batch] * width for row_idx in range(width)]
    low_imag = [[zero_batch] * width for row_idx in range(width)]
    for col_idx in range(width):
        remain = gram_real[col_idx, col_idx] + ridge_term
        for mid_idx in range(col_idx):
            remain = remain - low_real[col_idx][mid_idx] * low_real[col_idx][mid_idx]
            remain = remain - low_imag[col_idx][mid_idx] * low_imag[col_idx][mid_idx]
        diag_val = jnp.sqrt(remain)
        low_real[col_idx][col_idx] = diag_val
        for row_idx in range(col_idx + 1, width):
            sum_real = gram_real[row_idx, col_idx]
            sum_imag = gram_imag[row_idx, col_idx]
            for mid_idx in range(col_idx):
                left_real = low_real[row_idx][mid_idx]
                left_imag = low_imag[row_idx][mid_idx]
                right_real = low_real[col_idx][mid_idx]
                right_imag = low_imag[col_idx][mid_idx]
                sum_real = sum_real - (left_real * right_real + left_imag * right_imag)
                sum_imag = sum_imag - (left_imag * right_real - left_real * right_imag)
            low_real[row_idx][col_idx] = sum_real / diag_val
            low_imag[row_idx][col_idx] = sum_imag / diag_val
    inv_real = [[zero_batch] * width for row_idx in range(width)]
    inv_imag = [[zero_batch] * width for row_idx in range(width)]
    for col_idx in range(width):
        inv_real[col_idx][col_idx] = 1.0 / low_real[col_idx][col_idx]
        for row_idx in range(col_idx + 1, width):
            sum_real = zero_batch
            sum_imag = zero_batch
            for mid_idx in range(col_idx, row_idx):
                left_real = low_real[row_idx][mid_idx]
                left_imag = low_imag[row_idx][mid_idx]
                right_real = inv_real[mid_idx][col_idx]
                right_imag = inv_imag[mid_idx][col_idx]
                sum_real = sum_real + left_real * right_real - left_imag * right_imag
                sum_imag = sum_imag + left_real * right_imag + left_imag * right_real
            inv_real[row_idx][col_idx] = -sum_real / low_real[row_idx][row_idx]
            inv_imag[row_idx][col_idx] = -sum_imag / low_real[row_idx][row_idx]
    map_real = jnp.stack(
        [
            jnp.stack([inv_real[w_idx][v_idx] for w_idx in range(width)], axis=-1)
            for v_idx in range(width)
        ],
        axis=-2,
    )
    map_imag = -jnp.stack(
        [
            jnp.stack([inv_imag[w_idx][v_idx] for w_idx in range(width)], axis=-1)
            for v_idx in range(width)
        ],
        axis=-2,
    )
    mixing = jnp.stack(
        [jnp.stack([map_real, map_imag], axis=3), jnp.stack([-map_imag, map_real], axis=3)], axis=2
    )
    return jnp.einsum("nkvcas,nkavbw->nkwcbs", blocks, mixing, precision=top_precision)


def two_passes(blocks):
    return factor_pass(factor_pass(blocks))


def arrange(lattice, row_count, agg_edge):
    vector_count = lattice.shape[3]
    comp_count = lattice.shape[4]
    x_sites = lattice.shape[6]
    groups = x_sites // agg_edge
    pieces = lattice.reshape(
        row_count, agg_edge, agg_edge, vector_count, 2, comp_count // 2, 2, groups, agg_edge
    )
    pieces = pieces.transpose(7, 4, 3, 5, 6, 0, 1, 2, 8)
    return pieces.reshape(
        groups, 2, vector_count, comp_count // 2, 2, row_count * agg_edge * agg_edge * agg_edge
    )


def invert(slot_row):
    places = jnp.arange(slot_row.shape[0], dtype=jnp.int32)
    return jnp.sum(jnp.where(slot_row[None, :] == places[:, None], places[None, :], 0), axis=1)


def per_device_general(near_null, offsets, owner_slot):
    agg_edge = near_null.shape[0]
    rim_rows = agg_edge - 1
    from_z = from_behind(near_null[:, :rim_rows], "gz", -1)
    lattice = lax.dynamic_slice_in_dim(
        jnp.concatenate([near_null, from_z], axis=1), offsets[1], agg_edge, 1
    )
    from_y = from_behind(lattice[:, :, :rim_rows], "gy", -1)
    lattice = lax.dynamic_slice_in_dim(
        jnp.concatenate([lattice, from_y], axis=2), offsets[2], agg_edge, 2
    )
    x_sites = lattice.shape[5] // 2
    lattice = lattice.reshape(lattice.shape[:5] + (2, x_sites))
    lattice = lax.dynamic_slice_in_dim(
        jnp.concatenate([lattice, lattice], axis=6), offsets[3], x_sites, 6
    )
    slot_row = owner_slot.reshape(-1)
    source_of = invert(slot_row)
    from_t = from_behind(lattice[:rim_rows], "ta", -1)
    lattice = lax.dynamic_slice_in_dim(
        jnp.concatenate([lattice, from_t], axis=0), offsets[0], agg_edge, 0
    )
    tiles = arrange(lattice, agg_edge, agg_edge)
    packed = jnp.take(tiles, source_of, axis=0)
    result = two_passes(lax.all_to_all(packed, "ta", split_axis=0, concat_axis=0, tiled=True))
    return result


def solution(mesh):
    pair = mesh.shape["ta"] == 2 and mesh.shape["gz"] > 1 and mesh.shape["gy"] > 1
    return jax.shard_map(
        per_device_pair if pair else per_device_general,
        mesh=mesh,
        in_specs=(P("ta", "gz", "gy", None, None, None), P(), P("ta", "gz", "gy", None)),
        out_specs=P(("ta", "gz", "gy"), None, None, None, None, None),
        check_vma=False,
    )
```

```python
import functools

import jax
import jax.numpy as jnp
from jax import lax
from jax.experimental import pallas as pl
from jax.experimental.pallas import tpu as pltpu
from jax.sharding import PartitionSpec as P

MAX_OFFSET = 3
LEAD = 4
GRAM_PITCH = 24
MIX_PITCH = 40
MESH_ID = pl.DeviceIdType.MESH


def split(x):
    high = x.astype(jnp.bfloat16)
    return high, (x - high.astype(jnp.float32)).astype(jnp.bfloat16)


def exchange_kernel(
    oz,
    oy,
    pieces,
    vectors,
    offset_ref,
    slot_ref,
    near_ref,
    owned,
    total,
    raw,
    home,
    side,
    sent,
    other_slot,
    lane_from,
    in_sem,
    slot_sem,
    side_sem,
    home_sem,
    sent_sem,
    got_sem,
):
    edge = raw.shape[0]
    rows, lanes = home.shape[3:]
    chunk = rows // pieces
    count = edge * edge
    half = count // 2
    x_sites = lanes // 2
    me = lax.axis_index("ta")
    z_len, y_len = lax.axis_size("gz"), lax.axis_size("gy")
    z_at, y_at = lax.axis_index("gz"), lax.axis_index("gy")
    z_down, z_up = lax.rem(z_at + z_len - 1, z_len), lax.rem(z_at + 1, z_len)
    y_down, y_up = lax.rem(y_at + y_len - 1, y_len), lax.rem(y_at + 1, y_len)
    partner = {"ta": 1 - me}

    def in_copy(t, r):
        at = pl.ds(pl.multiple_of(r * chunk * edge, chunk * edge), chunk * edge)
        return pltpu.make_async_copy(near_ref.at[t, :, at], raw.at[t, :, at], in_sem.at[t, r])

    def start_in(i, carry):
        in_copy(i // pieces, i % pieces).start()
        return carry

    lax.fori_loop(0, edge * pieces, start_in, 0)

    barrier = pltpu.get_barrier_semaphore()
    greeted = [
        {"gz": z_down},
        {"gy": y_down},
        {"gz": z_down, "gy": y_down},
        {"gz": z_up},
        {"gy": y_up},
        {"gz": z_up, "gy": y_up},
        partner,
    ]
    for target in greeted:
        pl.semaphore_signal(barrier, inc=1, device_id=target, device_id_type=MESH_ID)
    pl.semaphore_wait(barrier, len(greeted))

    slot_copy = pltpu.make_async_remote_copy(
        src_ref=slot_ref,
        dst_ref=other_slot,
        send_sem=slot_sem.at[0],
        recv_sem=slot_sem.at[1],
        device_id=partner,
        device_id_type=MESH_ID,
    )
    slot_copy.start()

    near_z, far_z = (0, edge - oz), (edge - oz, oz)
    near_y, far_y = (0, edge - oy), (edge - oy, oy)
    parts = [
        (near_z, far_y, {"gy": y_down}),
        (far_z, far_y, {"gz": z_down, "gy": y_down}),
        (far_z, near_y, {"gz": z_down}),
    ]

    def part_copies(t, r):
        at = pl.ds(pl.multiple_of(r * chunk, chunk), chunk)
        made = []
        for n, ((z0, zn), (y0, yn), target) in enumerate(parts):
            made.append(
                pltpu.make_async_remote_copy(
                    src_ref=side.at[t, pl.ds(z0, zn), pl.ds(y0, yn), at],
                    dst_ref=home.at[t, pl.ds(z0, zn), pl.ds(y0, yn), at],
                    send_sem=side_sem.at[n, t, r],
                    recv_sem=home_sem.at[n, t, r],
                    device_id=target,
                    device_id_type=MESH_ID,
                )
            )
        return made

    def sent_copy(t, r):
        at = pl.ds(pl.multiple_of(r * chunk, chunk), chunk)
        return pltpu.make_async_remote_copy(
            src_ref=sent.at[t, :, at],
            dst_ref=owned.at[1, t, :, at],
            send_sem=sent_sem.at[t, r],
            recv_sem=got_sem.at[t, r],
            device_id=partner,
            device_id_type=MESH_ID,
        )

    def pack_piece(t, r):
        start = pl.multiple_of(r * chunk, chunk)
        for z in range(edge):
            for y in range(edge):
                target = home if z >= oz and y >= oy else side
                target[t, (z - oz) % edge, (y - oy) % edge, pl.ds(start, chunk), :] = raw[
                    t, z, pl.ds(start * edge + y, chunk, stride=edge), :
                ]

    def send_parts(t, r):
        for copy in part_copies(t, r):
            copy.start()

    def pack_next(i):
        t, r = i // pieces, i % pieces
        in_copy(t, r).wait()
        pack_piece(t, r)
        send_parts(t, r)

    def pack_first(i, carry):
        pack_next(i)
        return carry

    lead = min(LEAD, edge * pieces)
    lax.fori_loop(0, lead, pack_first, 0)
    total[...] = jnp.zeros_like(total)

    lane = lax.broadcasted_iota(jnp.int32, (8, lanes), 1)
    group = edge.bit_length() - 1
    wanted = ((lane >> group) & (count - 1)) ^ (me * half)

    def lanes_of(slots):
        found = jnp.zeros((8, lanes), jnp.int32)
        for j in range(count):
            slot = jnp.broadcast_to(slots[0:1, j : j + 1], (8, lanes))
            found = jnp.where(slot == wanted, j, found)
        x = (found * edge + (lane & (edge - 1)) + offset_ref[3]) & (x_sites - 1)
        return (lane & x_sites) + x

    lane_from[0] = lanes_of(slot_ref[...])
    slot_copy.wait()
    lane_from[1] = lanes_of(other_slot[...])

    def regroup_piece(t, r):
        start = pl.multiple_of(r * chunk, chunk)
        moved = jnp.where(t >= offset_ref[0], lane_from[0], lane_from[1])
        for g in range(chunk // 8):
            at = pl.ds(pl.multiple_of(start + g * 8, 8), 8)
            units = [
                jnp.take_along_axis(
                    home[t, u // edge, u % edge, at, :], moved, axis=1, mode="promise_in_bounds"
                )
                for u in range(count)
            ]
            bit = 1
            while bit < count:
                step = bit * edge
                high = (lane & step) != 0
                fresh = list(units)
                for u in range(count):
                    if not u & bit:
                        low_unit, high_unit = units[u], units[u + bit]
                        fresh[u] = jnp.where(high, pltpu.roll(high_unit, step, 1), low_unit)
                        fresh[u + bit] = jnp.where(
                            high, high_unit, pltpu.roll(low_unit, lanes - step, 1)
                        )
                units = fresh
                bit *= 2
            for j in range(half):
                sent[t, j, at, :] = units[half + j]
            for j in range(half):
                owned[0, t, j, at, :] = units[j]

    comps = rows // vectors
    kinds = comps // 2
    padded = 16
    pitch = total.shape[0] // (4 * half)
    low = lax.broadcasted_iota(jnp.int32, (padded, lanes), 1) < x_sites
    zeros = jnp.zeros((padded - vectors, lanes), jnp.float32)

    def gram_row(source, t, ours):
        def gram_of(q, h):
            values = [[], [], [], []]
            for k in range(kinds):
                piece = owned[source, t, q, pl.ds(h * kinds + k, vectors, stride=comps), :]
                piece = jnp.concatenate([piece, zeros], axis=0)
                turned = pltpu.roll(piece, x_sites, 1)
                turned = jnp.where(low, turned, -turned)
                for n, value in enumerate(split(piece) + split(turned)):
                    values[n].append(value)
            both = jnp.concatenate([jnp.concatenate(v, axis=1) for v in values], axis=0)
            products = lax.dot_general(
                both[: 2 * padded],
                both,
                (((1,), (1,)), ((), ())),
                preferred_element_type=jnp.float32,
            )
            products = products[:padded] + products[padded:]
            for side_of, value in enumerate(
                (jnp.where(ours, products, 0.0), jnp.where(ours, 0.0, products))
            ):
                start = ((side_of * half + q) * 2 + h) * pitch
                at = pl.ds(pl.multiple_of(start, 8), padded)
                total[at, : 4 * padded] += value

        def body(i, carry):
            for q in range(2):
                for h in range(2):
                    gram_of(i * 2 + q, h)
            return carry

        lax.fori_loop(0, half // 2, body, 0)

    def take_got(t):
        def body(r, carry):
            sent_copy(t, r).wait_recv()
            return carry

        lax.fori_loop(0, pieces, body, 0)
        gram_row(1, t, t < offset_ref[0])

    def regroup_row(t, carry):
        def body(r, inner):
            @pl.when(t * pieces + r + lead < edge * pieces)
            def _():
                pack_next(t * pieces + r + lead)

            for copy in part_copies(t, r):
                copy.wait_recv()
            regroup_piece(t, r)
            sent_copy(t, r).start()
            return inner

        lax.fori_loop(0, pieces, body, 0)
        gram_row(0, t, t >= offset_ref[0])

        @pl.when(t >= 1)
        def _():
            take_got(t - 1)

        return carry

    lax.fori_loop(0, edge, regroup_row, 0)
    take_got(edge - 1)

    def finish_row(t, carry):
        def body(r, inner):
            for copy in part_copies(t, r):
                copy.wait_send()
            sent_copy(t, r).wait_send()
            return inner

        return lax.fori_loop(0, pieces, body, carry)

    lax.fori_loop(0, edge, finish_row, 0)


def exchange(oz, oy, call_id, vectors, offsets, slots, lattice):
    edge, _, all_rows, lanes = lattice.shape
    rows = all_rows // edge
    pieces = max(p for p in range(1, 7) if rows % (8 * p) == 0)
    half = edge * edge // 2
    size = lattice.size
    block = (edge, half, rows, lanes)
    whole = (edge, edge, edge, rows, lanes)
    sums = (4 * half * GRAM_PITCH, lanes)
    return pl.pallas_call(
        functools.partial(exchange_kernel, oz, oy, pieces, vectors),
        in_specs=[
            pl.BlockSpec(memory_space=pltpu.SMEM),
            pl.BlockSpec(memory_space=pltpu.VMEM),
            pl.BlockSpec(memory_space=pl.ANY),
        ],
        out_specs=[pl.BlockSpec(memory_space=pltpu.VMEM)] * 2,
        out_shape=[pltpu.VMEM((2,) + block, jnp.float32), pltpu.VMEM(sums, jnp.float32)],
        scratch_shapes=[
            pltpu.VMEM(lattice.shape, jnp.float32),
            pltpu.VMEM(whole, jnp.float32),
            pltpu.VMEM(whole, jnp.float32),
            pltpu.VMEM(block, jnp.float32),
            pltpu.VMEM(slots.shape, jnp.int32),
            pltpu.VMEM((2, 8, lanes), jnp.int32),
            pltpu.SemaphoreType.DMA((edge, pieces)),
            pltpu.SemaphoreType.DMA((2,)),
            pltpu.SemaphoreType.DMA((3, edge, pieces)),
            pltpu.SemaphoreType.DMA((3, edge, pieces)),
            pltpu.SemaphoreType.DMA((edge, pieces)),
            pltpu.SemaphoreType.DMA((edge, pieces)),
        ],
        compiler_params=pltpu.CompilerParams(
            collective_id=call_id,
            has_side_effects=True,
            vmem_limit_bytes=20 * 1024 * 1024,
        ),
        cost_estimate=pl.CostEstimate(flops=size * 10, bytes_accessed=size * 9, transcendentals=0),
    )(offsets, slots, lattice)


def matmul_rows(left, right):
    out = []
    for v in range(len(left)):
        real = imag = None
        for m in range(v + 1):
            a = left[v][0][m : m + 1, :]
            b = left[v][1][m : m + 1, :]
            r, i = right[m]
            term_real, term_imag = a * r - b * i, a * i + b * r
            real = term_real if real is None else real + term_real
            imag = term_imag if imag is None else imag + term_imag
        out.append((real, imag))
    return out


def invert_factor(gram, width):
    row_of = lax.broadcasted_iota(jnp.int32, gram[0][0].shape, 0)
    mean = gram[0][0][0:1, :]
    for v in range(1, width):
        mean = mean + gram[v][0][v : v + 1, :]
    ridge = 0.05 * (mean / width + 1e-06)
    rows = [(jnp.where(row_of == v, r + ridge, r), i) for v, (r, i) in enumerate(gram)]
    zero = jnp.zeros_like(rows[0][0])
    inverse = [(jnp.where(row_of == v, 1.0, zero), zero) for v in range(width)]
    for k in range(width):
        scale = 1.0 / jnp.sqrt(rows[k][0][k : k + 1, :])
        pivot = (rows[k][0] * scale, rows[k][1] * scale)
        known = (inverse[k][0] * scale, inverse[k][1] * scale)
        inverse[k] = known
        for v in range(k + 1, width):
            a = pivot[0][v : v + 1, :]
            b = -pivot[1][v : v + 1, :]
            r, i = rows[v]
            rows[v] = (r - (a * pivot[0] - b * pivot[1]), i - (a * pivot[1] + b * pivot[0]))
            r, i = inverse[v]
            inverse[v] = (r - (a * known[0] - b * known[1]), i - (a * known[1] + b * known[0]))
    return inverse


def factor_kernel(
    vectors,
    offset_ref,
    owned,
    gram,
    out_ref,
    stage,
    mix,
    turn,
    out_sem,
):
    _, edge, per_home, unit_rows, lanes = owned.shape
    comps = unit_rows // vectors
    kinds = comps // 2
    count = 2 * per_home
    batch = 2 * count
    padded = 16
    mid = lanes // 2
    norm = 1.0 / (kinds * edge**4)
    me = lax.axis_index("ta")
    ot = offset_ref[0]

    first = []
    for v in range(vectors):
        block = gram[pl.ds(v, batch, stride=GRAM_PITCH), :].T * norm
        first.append(
            (
                block[:padded] + block[padded : 2 * padded],
                block[2 * padded : 3 * padded] + block[3 * padded : 4 * padded],
            )
        )
    inverse = invert_factor(first, vectors)
    moved = matmul_rows(inverse, first)
    for v in range(padded):
        for w in range(2):
            turn[w, v * padded : (v + 1) * padded, :] = (
                moved[v][w] if v < vectors else jnp.zeros((padded, batch), jnp.float32)
            )
    flipped = [
        (turn[0, pl.ds(m, padded, stride=padded), :], -turn[1, pl.ds(m, padded, stride=padded), :])
        for m in range(vectors)
    ]
    second = matmul_rows(inverse, flipped)
    final = matmul_rows(invert_factor(second, vectors), inverse)
    rest = jnp.zeros((lanes - 6 * padded, batch), jnp.float32)
    for w in range(padded):
        if w < vectors:
            real, imag = final[w]
            blocks = ([real, imag] * 3 + [rest], [-imag, real] * 3 + [rest])
            for n, block in enumerate(blocks):
                at = pl.ds(n * padded + w, batch, stride=MIX_PITCH)
                mix[at, :] = jnp.concatenate(block, axis=0).T
        else:
            for n in range(2):
                at = pl.ds(n * padded + w, batch, stride=MIX_PITCH)
                mix[at, :] = jnp.zeros((batch, lanes), jnp.float32)

    zeros = jnp.zeros((padded - vectors, lanes), jnp.float32)
    low = lax.broadcasted_iota(jnp.int32, (padded, lanes), 1) < mid

    def out_copy(n):
        at = (me ^ (n // per_home)) * per_home + n % per_home
        return pltpu.make_async_copy(stage.at[n], out_ref.at[at], out_sem.at[n])

    is_high = lax.broadcasted_iota(jnp.int32, (2 * padded, lanes), 1) < 4 * padded

    def apply_to(n):
        at_home, slot = n // per_home, n % per_home
        rows_t = [(t + ot) & (edge - 1) for t in range(edge)]
        sources = [jnp.where(t >= ot, at_home, 1 - at_home) for t in rows_t]
        for h in range(2):
            start = pl.multiple_of((n * 2 + h) * MIX_PITCH, 8)
            mixing = mix[pl.ds(start, 2 * padded), :]
            high = mixing.astype(jnp.bfloat16).astype(jnp.float32)
            left = jnp.where(is_high, high, mixing - high).astype(jnp.bfloat16)[:, : 6 * padded]
            for k in range(kinds):
                right = []
                for s in range(edge // 2):
                    one, two = (
                        jnp.concatenate(
                            [
                                owned[
                                    sources[2 * s + w],
                                    rows_t[2 * s + w],
                                    slot,
                                    pl.ds(h * kinds + k, vectors, stride=comps),
                                    :,
                                ],
                                zeros,
                            ],
                            axis=0,
                        )
                        for w in range(2)
                    )
                    real_high, real_low = split(jnp.where(low, one, pltpu.roll(two, mid, 1)))
                    imag_high, imag_low = split(jnp.where(low, pltpu.roll(one, mid, 1), two))
                    right.append(
                        jnp.concatenate(
                            [real_high, imag_high, real_low, imag_low, real_high, imag_high], axis=0
                        )
                    )
                made = jnp.dot(
                    left, jnp.concatenate(right, axis=1), preferred_element_type=jnp.float32
                )
                for s in range(edge // 2):
                    for w in range(2):
                        at = pl.ds(k * edge + 2 * s + w, vectors, stride=kinds * edge)
                        stage[n, h, at, :] = made[
                            w * padded : w * padded + vectors, s * lanes : (s + 1) * lanes
                        ]
        out_copy(n).start()

    def apply_pair(i, carry):
        apply_to(2 * i)
        apply_to(2 * i + 1)
        return carry

    lax.fori_loop(0, count // 2, apply_pair, 0)

    def finish(n, carry):
        out_copy(n).wait()
        return carry

    lax.fori_loop(0, count, finish, 0)


def factor(vectors, offsets, owned, gram):
    _, edge, per_home, unit_rows, lanes = owned.shape
    comps = unit_rows // vectors
    count = 2 * per_home
    batch = 2 * count
    out_rows = vectors * comps // 2 * edge
    size = count * edge * unit_rows * lanes
    return pl.pallas_call(
        functools.partial(factor_kernel, vectors),
        in_specs=[pl.BlockSpec(memory_space=pltpu.SMEM)]
        + [pl.BlockSpec(memory_space=pltpu.VMEM)] * 2,
        out_specs=pl.BlockSpec(memory_space=pl.ANY),
        out_shape=jax.ShapeDtypeStruct((count, 2, out_rows, lanes), jnp.float32),
        scratch_shapes=[
            pltpu.VMEM((count, 2, out_rows, lanes), jnp.float32),
            pltpu.VMEM((batch * MIX_PITCH, lanes), jnp.float32),
            pltpu.VMEM((2, 16 * 16, batch), jnp.float32),
            pltpu.SemaphoreType.DMA((count,)),
        ],
        compiler_params=pltpu.CompilerParams(vmem_limit_bytes=56 * 1024 * 1024),
        cost_estimate=pl.CostEstimate(flops=size * 100, bytes_accessed=size * 8, transcendentals=0),
    )(
        offsets,
        pltpu.with_memory_space_constraint(owned, pltpu.VMEM),
        pltpu.with_memory_space_constraint(gram, pltpu.VMEM),
    )


def per_device_pair(near_null, offsets, owner_slot):
    edge = near_null.shape[0]
    vectors, comps = near_null.shape[3:5]
    slots = owner_slot.reshape(1, -1)
    lattice = near_null.transpose(0, 1, 3, 4, 2, 5).reshape(
        edge, near_null.shape[1], -1, near_null.shape[5]
    )
    def both(oz, oy, offsets, slots, lattice):
        call_id = (oz - 1) * MAX_OFFSET + oy - 1
        owned, gram = exchange(oz, oy, call_id, vectors, offsets, slots, lattice)
        made = factor(vectors, offsets, owned, gram)
        count, _, _, lanes = made.shape
        made = made.reshape(count, 2, vectors, comps // 2, edge // 2, 2, lanes)
        return made.transpose(0, 1, 2, 3, 5, 4, 6).reshape(
            count, 2, vectors, comps // 2, 2, edge // 2 * lanes
        )

    branches = [
        functools.partial(both, oz, oy)
        for oz in range(1, MAX_OFFSET + 1)
        for oy in range(1, MAX_OFFSET + 1)
    ]
    which = (offsets[1] - 1) * MAX_OFFSET + offsets[2] - 1
    return lax.switch(which, branches, offsets, slots, lattice)


ridge_scale = 0.05
top_precision = lax.Precision.HIGHEST


def from_behind(array, axis, by):
    length = lax.axis_size(axis)
    return lax.ppermute(array, axis, [(i, (i + by) % length) for i in range(length)])


def factor_pass(blocks):
    norm_count = blocks.shape[3] * blocks.shape[5]
    products = (
        jnp.einsum("nkvcas,nkwcbs->nkavbw", blocks, blocks, precision=top_precision) / norm_count
    )
    gram_real = products[:, :, 0, :, 0, :] + products[:, :, 1, :, 1, :]
    gram_imag = products[:, :, 0, :, 1, :] - products[:, :, 1, :, 0, :]
    width = gram_real.shape[-1]
    diag_mean = jnp.mean(jnp.diagonal(gram_real, axis1=2, axis2=3), axis=-1)
    ridge_term = ridge_scale * (diag_mean + 1e-06)
    gram_real = jnp.moveaxis(gram_real, (2, 3), (0, 1))
    gram_imag = jnp.moveaxis(gram_imag, (2, 3), (0, 1))
    zero_batch = jnp.zeros_like(ridge_term)
    low_real = [[zero_batch] * width for row_idx in range(width)]
    low_imag = [[zero_batch] * width for row_idx in range(width)]
    for col_idx in range(width):
        remain = gram_real[col_idx, col_idx] + ridge_term
        for mid_idx in range(col_idx):
            remain = remain - low_real[col_idx][mid_idx] * low_real[col_idx][mid_idx]
            remain = remain - low_imag[col_idx][mid_idx] * low_imag[col_idx][mid_idx]
        diag_val = jnp.sqrt(remain)
        low_real[col_idx][col_idx] = diag_val
        for row_idx in range(col_idx + 1, width):
            sum_real = gram_real[row_idx, col_idx]
            sum_imag = gram_imag[row_idx, col_idx]
            for mid_idx in range(col_idx):
                left_real = low_real[row_idx][mid_idx]
                left_imag = low_imag[row_idx][mid_idx]
                right_real = low_real[col_idx][mid_idx]
                right_imag = low_imag[col_idx][mid_idx]
                sum_real = sum_real - (left_real * right_real + left_imag * right_imag)
                sum_imag = sum_imag - (left_imag * right_real - left_real * right_imag)
            low_real[row_idx][col_idx] = sum_real / diag_val
            low_imag[row_idx][col_idx] = sum_imag / diag_val
    inv_real = [[zero_batch] * width for row_idx in range(width)]
    inv_imag = [[zero_batch] * width for row_idx in range(width)]
    for col_idx in range(width):
        inv_real[col_idx][col_idx] = 1.0 / low_real[col_idx][col_idx]
        for row_idx in range(col_idx + 1, width):
            sum_real = zero_batch
            sum_imag = zero_batch
            for mid_idx in range(col_idx, row_idx):
                left_real = low_real[row_idx][mid_idx]
                left_imag = low_imag[row_idx][mid_idx]
                right_real = inv_real[mid_idx][col_idx]
                right_imag = inv_imag[mid_idx][col_idx]
                sum_real = sum_real + left_real * right_real - left_imag * right_imag
                sum_imag = sum_imag + left_real * right_imag + left_imag * right_real
            inv_real[row_idx][col_idx] = -sum_real / low_real[row_idx][row_idx]
            inv_imag[row_idx][col_idx] = -sum_imag / low_real[row_idx][row_idx]
    map_real = jnp.stack(
        [
            jnp.stack([inv_real[w_idx][v_idx] for w_idx in range(width)], axis=-1)
            for v_idx in range(width)
        ],
        axis=-2,
    )
    map_imag = -jnp.stack(
        [
            jnp.stack([inv_imag[w_idx][v_idx] for w_idx in range(width)], axis=-1)
            for v_idx in range(width)
        ],
        axis=-2,
    )
    mixing = jnp.stack(
        [jnp.stack([map_real, map_imag], axis=3), jnp.stack([-map_imag, map_real], axis=3)], axis=2
    )
    return jnp.einsum("nkvcas,nkavbw->nkwcbs", blocks, mixing, precision=top_precision)


def two_passes(blocks):
    return factor_pass(factor_pass(blocks))


def arrange(lattice, row_count, agg_edge):
    vector_count = lattice.shape[3]
    comp_count = lattice.shape[4]
    x_sites = lattice.shape[6]
    groups = x_sites // agg_edge
    pieces = lattice.reshape(
        row_count, agg_edge, agg_edge, vector_count, 2, comp_count // 2, 2, groups, agg_edge
    )
    pieces = pieces.transpose(7, 4, 3, 5, 6, 0, 1, 2, 8)
    return pieces.reshape(
        groups, 2, vector_count, comp_count // 2, 2, row_count * agg_edge * agg_edge * agg_edge
    )


def invert(slot_row):
    places = jnp.arange(slot_row.shape[0], dtype=jnp.int32)
    return jnp.sum(jnp.where(slot_row[None, :] == places[:, None], places[None, :], 0), axis=1)


def per_device_general(near_null, offsets, owner_slot):
    agg_edge = near_null.shape[0]
    rim_rows = agg_edge - 1
    from_z = from_behind(near_null[:, :rim_rows], "gz", -1)
    lattice = lax.dynamic_slice_in_dim(
        jnp.concatenate([near_null, from_z], axis=1), offsets[1], agg_edge, 1
    )
    from_y = from_behind(lattice[:, :, :rim_rows], "gy", -1)
    lattice = lax.dynamic_slice_in_dim(
        jnp.concatenate([lattice, from_y], axis=2), offsets[2], agg_edge, 2
    )
    x_sites = lattice.shape[5] // 2
    lattice = lattice.reshape(lattice.shape[:5] + (2, x_sites))
    lattice = lax.dynamic_slice_in_dim(
        jnp.concatenate([lattice, lattice], axis=6), offsets[3], x_sites, 6
    )
    slot_row = owner_slot.reshape(-1)
    source_of = invert(slot_row)
    from_t = from_behind(lattice[:rim_rows], "ta", -1)
    lattice = lax.dynamic_slice_in_dim(
        jnp.concatenate([lattice, from_t], axis=0), offsets[0], agg_edge, 0
    )
    tiles = arrange(lattice, agg_edge, agg_edge)
    packed = jnp.take(tiles, source_of, axis=0)
    result = two_passes(lax.all_to_all(packed, "ta", split_axis=0, concat_axis=0, tiled=True))
    return result


def solution(mesh):
    pair = mesh.shape["ta"] == 2 and mesh.shape["gz"] > 1 and mesh.shape["gy"] > 1
    return jax.shard_map(
        per_device_pair if pair else per_device_general,
        mesh=mesh,
        in_specs=(P("ta", "gz", "gy", None, None, None), P(), P("ta", "gz", "gy", None)),
        out_specs=P(("ta", "gz", "gy"), None, None, None, None, None),
        check_vma=False,
    )
```

```python
import functools

import jax
import jax.numpy as jnp
from jax import lax
from jax.experimental import pallas as pl
from jax.experimental.pallas import tpu as pltpu
from jax.sharding import PartitionSpec as P

MAX_OFFSET = 3
LEAD = 4
GRAM_PITCH = 24
MIX_PITCH = 40
MESH_ID = pl.DeviceIdType.MESH


def split(x):
    high = x.astype(jnp.bfloat16)
    return high, (x - high.astype(jnp.float32)).astype(jnp.bfloat16)


def exchange_kernel(
    oz,
    oy,
    pieces,
    vectors,
    offset_ref,
    slot_ref,
    near_ref,
    owned,
    total,
    raw,
    home,
    side,
    sent,
    other_slot,
    lane_from,
    in_sem,
    slot_sem,
    side_sem,
    home_sem,
    sent_sem,
    got_sem,
):
    edge = raw.shape[0]
    rows, lanes = home.shape[3:]
    chunk = rows // pieces
    count = edge * edge
    half = count // 2
    x_sites = lanes // 2
    me = lax.axis_index("ta")
    z_len, y_len = lax.axis_size("gz"), lax.axis_size("gy")
    z_at, y_at = lax.axis_index("gz"), lax.axis_index("gy")
    z_down, z_up = lax.rem(z_at + z_len - 1, z_len), lax.rem(z_at + 1, z_len)
    y_down, y_up = lax.rem(y_at + y_len - 1, y_len), lax.rem(y_at + 1, y_len)
    partner = {"ta": 1 - me}

    def in_copy(t, r):
        at = pl.ds(pl.multiple_of(r * chunk * edge, chunk * edge), chunk * edge)
        return pltpu.make_async_copy(near_ref.at[t, :, at], raw.at[t, :, at], in_sem.at[t, r])

    def start_in(i, carry):
        in_copy(i // pieces, i % pieces).start()
        return carry

    lax.fori_loop(0, edge * pieces, start_in, 0)

    barrier = pltpu.get_barrier_semaphore()
    greeted = [
        {"gz": z_down},
        {"gy": y_down},
        {"gz": z_down, "gy": y_down},
        {"gz": z_up},
        {"gy": y_up},
        {"gz": z_up, "gy": y_up},
        partner,
    ]
    for target in greeted:
        pl.semaphore_signal(barrier, inc=1, device_id=target, device_id_type=MESH_ID)
    pl.semaphore_wait(barrier, len(greeted))

    slot_copy = pltpu.make_async_remote_copy(
        src_ref=slot_ref,
        dst_ref=other_slot,
        send_sem=slot_sem.at[0],
        recv_sem=slot_sem.at[1],
        device_id=partner,
        device_id_type=MESH_ID,
    )
    slot_copy.start()

    near_z, far_z = (0, edge - oz), (edge - oz, oz)
    near_y, far_y = (0, edge - oy), (edge - oy, oy)
    parts = [
        (near_z, far_y, {"gy": y_down}),
        (far_z, far_y, {"gz": z_down, "gy": y_down}),
        (far_z, near_y, {"gz": z_down}),
    ]

    def part_copies(t, r):
        at = pl.ds(pl.multiple_of(r * chunk, chunk), chunk)
        made = []
        for n, ((z0, zn), (y0, yn), target) in enumerate(parts):
            made.append(
                pltpu.make_async_remote_copy(
                    src_ref=side.at[t, pl.ds(z0, zn), pl.ds(y0, yn), at],
                    dst_ref=home.at[t, pl.ds(z0, zn), pl.ds(y0, yn), at],
                    send_sem=side_sem.at[n, t, r],
                    recv_sem=home_sem.at[n, t, r],
                    device_id=target,
                    device_id_type=MESH_ID,
                )
            )
        return made

    def sent_copy(t, r):
        at = pl.ds(pl.multiple_of(r * chunk, chunk), chunk)
        return pltpu.make_async_remote_copy(
            src_ref=sent.at[t, :, at],
            dst_ref=owned.at[1, t, :, at],
            send_sem=sent_sem.at[t, r],
            recv_sem=got_sem.at[t, r],
            device_id=partner,
            device_id_type=MESH_ID,
        )

    def pack_piece(t, r):
        start = pl.multiple_of(r * chunk, chunk)
        for z in range(edge):
            for y in range(edge):
                target = home if z >= oz and y >= oy else side
                target[t, (z - oz) % edge, (y - oy) % edge, pl.ds(start, chunk), :] = raw[
                    t, z, pl.ds(start * edge + y, chunk, stride=edge), :
                ]

    def send_parts(t, r):
        for copy in part_copies(t, r):
            copy.start()

    def pack_next(i):
        t, r = i // pieces, i % pieces
        in_copy(t, r).wait()
        pack_piece(t, r)
        send_parts(t, r)

    def pack_first(i, carry):
        pack_next(i)
        return carry

    lead = min(LEAD, edge * pieces)
    lax.fori_loop(0, lead, pack_first, 0)
    total[...] = jnp.zeros_like(total)

    lane = lax.broadcasted_iota(jnp.int32, (8, lanes), 1)
    group = edge.bit_length() - 1
    wanted = ((lane >> group) & (count - 1)) ^ (me * half)

    def lanes_of(slots):
        found = jnp.zeros((8, lanes), jnp.int32)
        for j in range(count):
            slot = jnp.broadcast_to(slots[0:1, j : j + 1], (8, lanes))
            found = jnp.where(slot == wanted, j, found)
        x = (found * edge + (lane & (edge - 1)) + offset_ref[3]) & (x_sites - 1)
        return (lane & x_sites) + x

    lane_from[0] = lanes_of(slot_ref[...])
    slot_copy.wait()
    lane_from[1] = lanes_of(other_slot[...])

    def regroup_piece(t, r):
        start = pl.multiple_of(r * chunk, chunk)
        moved = jnp.where(t >= offset_ref[0], lane_from[0], lane_from[1])
        for g in range(chunk // 8):
            at = pl.ds(pl.multiple_of(start + g * 8, 8), 8)
            units = [
                jnp.take_along_axis(
                    home[t, u // edge, u % edge, at, :], moved, axis=1, mode="promise_in_bounds"
                )
                for u in range(count)
            ]
            bit = 1
            while bit < count:
                step = bit * edge
                high = (lane & step) != 0
                fresh = list(units)
                for u in range(count):
                    if not u & bit:
                        low_unit, high_unit = units[u], units[u + bit]
                        fresh[u] = jnp.where(high, pltpu.roll(high_unit, step, 1), low_unit)
                        fresh[u + bit] = jnp.where(
                            high, high_unit, pltpu.roll(low_unit, lanes - step, 1)
                        )
                units = fresh
                bit *= 2
            for j in range(half):
                sent[t, j, at, :] = units[half + j]
            for j in range(half):
                owned[0, t, j, at, :] = units[j]

    comps = rows // vectors
    kinds = comps // 2
    padded = 16
    pitch = total.shape[0] // (4 * half)
    low = lax.broadcasted_iota(jnp.int32, (padded, lanes), 1) < x_sites
    zeros = jnp.zeros((padded - vectors, lanes), jnp.float32)

    def gram_row(source, t, ours):
        def gram_of(q, h):
            values = [[], [], [], []]
            for k in range(kinds):
                piece = owned[source, t, q, pl.ds(h * kinds + k, vectors, stride=comps), :]
                piece = jnp.concatenate([piece, zeros], axis=0)
                turned = pltpu.roll(piece, x_sites, 1)
                turned = jnp.where(low, turned, -turned)
                for n, value in enumerate(split(piece) + split(turned)):
                    values[n].append(value)
            both = jnp.concatenate([jnp.concatenate(v, axis=1) for v in values], axis=0)
            products = lax.dot_general(
                both[: 2 * padded],
                both,
                (((1,), (1,)), ((), ())),
                preferred_element_type=jnp.float32,
            )
            products = products[:padded] + products[padded:]
            for side_of, value in enumerate(
                (jnp.where(ours, products, 0.0), jnp.where(ours, 0.0, products))
            ):
                start = ((side_of * half + q) * 2 + h) * pitch
                at = pl.ds(pl.multiple_of(start, 8), padded)
                total[at, : 4 * padded] += value

        def body(i, carry):
            for q in range(2):
                for h in range(2):
                    gram_of(i * 2 + q, h)
            return carry

        lax.fori_loop(0, half // 2, body, 0)

    def take_got(t):
        def body(r, carry):
            sent_copy(t, r).wait_recv()
            return carry

        lax.fori_loop(0, pieces, body, 0)
        gram_row(1, t, t < offset_ref[0])

    def regroup_row(t, carry):
        def body(r, inner):
            @pl.when(t * pieces + r + lead < edge * pieces)
            def _():
                pack_next(t * pieces + r + lead)

            for copy in part_copies(t, r):
                copy.wait_recv()
            regroup_piece(t, r)
            sent_copy(t, r).start()
            return inner

        lax.fori_loop(0, pieces, body, 0)
        gram_row(0, t, t >= offset_ref[0])

        @pl.when(t >= 1)
        def _():
            take_got(t - 1)

        return carry

    lax.fori_loop(0, edge, regroup_row, 0)
    take_got(edge - 1)

    def finish_row(t, carry):
        def body(r, inner):
            for copy in part_copies(t, r):
                copy.wait_send()
            sent_copy(t, r).wait_send()
            return inner

        return lax.fori_loop(0, pieces, body, carry)

    lax.fori_loop(0, edge, finish_row, 0)


def exchange(oz, oy, call_id, vectors, offsets, slots, lattice):
    edge, _, all_rows, lanes = lattice.shape
    rows = all_rows // edge
    pieces = max(p for p in range(1, 7) if rows % (8 * p) == 0)
    half = edge * edge // 2
    size = lattice.size
    block = (edge, half, rows, lanes)
    whole = (edge, edge, edge, rows, lanes)
    sums = (4 * half * GRAM_PITCH, lanes)
    return pl.pallas_call(
        functools.partial(exchange_kernel, oz, oy, pieces, vectors),
        in_specs=[
            pl.BlockSpec(memory_space=pltpu.SMEM),
            pl.BlockSpec(memory_space=pltpu.VMEM),
            pl.BlockSpec(memory_space=pl.ANY),
        ],
        out_specs=[pl.BlockSpec(memory_space=pltpu.VMEM)] * 2,
        out_shape=[pltpu.VMEM((2,) + block, jnp.float32), pltpu.VMEM(sums, jnp.float32)],
        scratch_shapes=[
            pltpu.VMEM(lattice.shape, jnp.float32),
            pltpu.VMEM(whole, jnp.float32),
            pltpu.VMEM(whole, jnp.float32),
            pltpu.VMEM(block, jnp.float32),
            pltpu.VMEM(slots.shape, jnp.int32),
            pltpu.VMEM((2, 8, lanes), jnp.int32),
            pltpu.SemaphoreType.DMA((edge, pieces)),
            pltpu.SemaphoreType.DMA((2,)),
            pltpu.SemaphoreType.DMA((3, edge, pieces)),
            pltpu.SemaphoreType.DMA((3, edge, pieces)),
            pltpu.SemaphoreType.DMA((edge, pieces)),
            pltpu.SemaphoreType.DMA((edge, pieces)),
        ],
        compiler_params=pltpu.CompilerParams(
            collective_id=call_id,
            has_side_effects=True,
            vmem_limit_bytes=20 * 1024 * 1024,
        ),
        cost_estimate=pl.CostEstimate(flops=size * 10, bytes_accessed=size * 9, transcendentals=0),
    )(offsets, slots, lattice)


def matmul_rows(left, right):
    out = []
    for v in range(len(left)):
        real = imag = None
        for m in range(v + 1):
            a = left[v][0][m : m + 1, :]
            b = left[v][1][m : m + 1, :]
            r, i = right[m]
            term_real, term_imag = a * r - b * i, a * i + b * r
            real = term_real if real is None else real + term_real
            imag = term_imag if imag is None else imag + term_imag
        out.append((real, imag))
    return out


def invert_factor(gram, width):
    row_of = lax.broadcasted_iota(jnp.int32, gram[0][0].shape, 0)
    mean = gram[0][0][0:1, :]
    for v in range(1, width):
        mean = mean + gram[v][0][v : v + 1, :]
    ridge = 0.05 * (mean / width + 1e-06)
    rows = [(jnp.where(row_of == v, r + ridge, r), i) for v, (r, i) in enumerate(gram)]
    zero = jnp.zeros_like(rows[0][0])
    inverse = [(jnp.where(row_of == v, 1.0, zero), zero) for v in range(width)]
    for k in range(width):
        scale = 1.0 / jnp.sqrt(rows[k][0][k : k + 1, :])
        pivot = (rows[k][0] * scale, rows[k][1] * scale)
        known = (inverse[k][0] * scale, inverse[k][1] * scale)
        inverse[k] = known
        for v in range(k + 1, width):
            a = pivot[0][v : v + 1, :]
            b = -pivot[1][v : v + 1, :]
            r, i = rows[v]
            rows[v] = (r - (a * pivot[0] - b * pivot[1]), i - (a * pivot[1] + b * pivot[0]))
            r, i = inverse[v]
            inverse[v] = (r - (a * known[0] - b * known[1]), i - (a * known[1] + b * known[0]))
    return inverse


def factor_kernel(
    vectors,
    offset_ref,
    owned,
    gram,
    out_ref,
    stage,
    mix,
    turn,
    out_sem,
):
    _, edge, per_home, unit_rows, lanes = owned.shape
    comps = unit_rows // vectors
    kinds = comps // 2
    count = 2 * per_home
    batch = 2 * count
    padded = 16
    mid = lanes // 2
    norm = 1.0 / (kinds * edge**4)
    me = lax.axis_index("ta")
    ot = offset_ref[0]

    first = []
    for v in range(vectors):
        block = gram[pl.ds(v, batch, stride=GRAM_PITCH), :].T * norm
        first.append(
            (
                block[:padded] + block[padded : 2 * padded],
                block[2 * padded : 3 * padded] + block[3 * padded : 4 * padded],
            )
        )
    inverse = invert_factor(first, vectors)
    moved = matmul_rows(inverse, first)
    for v in range(padded):
        for w in range(2):
            turn[w, v * padded : (v + 1) * padded, :] = (
                moved[v][w] if v < vectors else jnp.zeros((padded, batch), jnp.float32)
            )
    flipped = [
        (turn[0, pl.ds(m, padded, stride=padded), :], -turn[1, pl.ds(m, padded, stride=padded), :])
        for m in range(vectors)
    ]
    second = matmul_rows(inverse, flipped)
    final = matmul_rows(invert_factor(second, vectors), inverse)
    rest = jnp.zeros((lanes - 6 * padded, batch), jnp.float32)
    for w in range(padded):
        if w < vectors:
            real, imag = final[w]
            blocks = ([real, imag] * 3 + [rest], [-imag, real] * 3 + [rest])
            for n, block in enumerate(blocks):
                at = pl.ds(n * padded + w, batch, stride=MIX_PITCH)
                mix[at, :] = jnp.concatenate(block, axis=0).T
        else:
            for n in range(2):
                at = pl.ds(n * padded + w, batch, stride=MIX_PITCH)
                mix[at, :] = jnp.zeros((batch, lanes), jnp.float32)

    zeros = jnp.zeros((padded - vectors, lanes), jnp.float32)
    low = lax.broadcasted_iota(jnp.int32, (padded, lanes), 1) < mid

    def out_copy(n):
        at = (me ^ (n // per_home)) * per_home + n % per_home
        return pltpu.make_async_copy(stage.at[n], out_ref.at[at], out_sem.at[n])

    is_high = lax.broadcasted_iota(jnp.int32, (2 * padded, lanes), 1) < 4 * padded

    def apply_to(n):
        at_home, slot = n // per_home, n % per_home
        rows_t = [(t + ot) & (edge - 1) for t in range(edge)]
        sources = [jnp.where(t >= ot, at_home, 1 - at_home) for t in rows_t]
        for h in range(2):
            start = pl.multiple_of((n * 2 + h) * MIX_PITCH, 8)
            mixing = mix[pl.ds(start, 2 * padded), :]
            high = mixing.astype(jnp.bfloat16).astype(jnp.float32)
            left = jnp.where(is_high, high, mixing - high).astype(jnp.bfloat16)[:, : 6 * padded]
            for k in range(kinds):
                right = []
                for s in range(edge // 2):
                    one, two = (
                        jnp.concatenate(
                            [
                                owned[
                                    sources[2 * s + w],
                                    rows_t[2 * s + w],
                                    slot,
                                    pl.ds(h * kinds + k, vectors, stride=comps),
                                    :,
                                ],
                                zeros,
                            ],
                            axis=0,
                        )
                        for w in range(2)
                    )
                    real_high, real_low = split(jnp.where(low, one, pltpu.roll(two, mid, 1)))
                    imag_high, imag_low = split(jnp.where(low, pltpu.roll(one, mid, 1), two))
                    right.append(
                        jnp.concatenate(
                            [real_high, imag_high, real_low, imag_low, real_high, imag_high], axis=0
                        )
                    )
                made = jnp.dot(
                    left, jnp.concatenate(right, axis=1), preferred_element_type=jnp.float32
                )
                for s in range(edge // 2):
                    for w in range(2):
                        at = pl.ds(k * edge + 2 * s + w, vectors, stride=kinds * edge)
                        stage[n, h, at, :] = made[
                            w * padded : w * padded + vectors, s * lanes : (s + 1) * lanes
                        ]
        out_copy(n).start()

    def apply_group(i, carry):
        for j in range(4):
            apply_to(4 * i + j)
        return carry

    lax.fori_loop(0, count // 4, apply_group, 0)

    def finish(n, carry):
        out_copy(n).wait()
        return carry

    lax.fori_loop(0, count, finish, 0)


def factor(vectors, offsets, owned, gram):
    _, edge, per_home, unit_rows, lanes = owned.shape
    comps = unit_rows // vectors
    count = 2 * per_home
    batch = 2 * count
    out_rows = vectors * comps // 2 * edge
    size = count * edge * unit_rows * lanes
    return pl.pallas_call(
        functools.partial(factor_kernel, vectors),
        in_specs=[pl.BlockSpec(memory_space=pltpu.SMEM)]
        + [pl.BlockSpec(memory_space=pltpu.VMEM)] * 2,
        out_specs=pl.BlockSpec(memory_space=pl.ANY),
        out_shape=jax.ShapeDtypeStruct((count, 2, out_rows, lanes), jnp.float32),
        scratch_shapes=[
            pltpu.VMEM((count, 2, out_rows, lanes), jnp.float32),
            pltpu.VMEM((batch * MIX_PITCH, lanes), jnp.float32),
            pltpu.VMEM((2, 16 * 16, batch), jnp.float32),
            pltpu.SemaphoreType.DMA((count,)),
        ],
        compiler_params=pltpu.CompilerParams(vmem_limit_bytes=56 * 1024 * 1024),
        cost_estimate=pl.CostEstimate(flops=size * 100, bytes_accessed=size * 8, transcendentals=0),
    )(
        offsets,
        pltpu.with_memory_space_constraint(owned, pltpu.VMEM),
        pltpu.with_memory_space_constraint(gram, pltpu.VMEM),
    )


def per_device_pair(near_null, offsets, owner_slot):
    edge = near_null.shape[0]
    vectors, comps = near_null.shape[3:5]
    slots = owner_slot.reshape(1, -1)
    lattice = near_null.transpose(0, 1, 3, 4, 2, 5).reshape(
        edge, near_null.shape[1], -1, near_null.shape[5]
    )
    def both(oz, oy, offsets, slots, lattice):
        call_id = (oz - 1) * MAX_OFFSET + oy - 1
        owned, gram = exchange(oz, oy, call_id, vectors, offsets, slots, lattice)
        made = factor(vectors, offsets, owned, gram)
        count, _, _, lanes = made.shape
        made = made.reshape(count, 2, vectors, comps // 2, edge // 2, 2, lanes)
        return made.transpose(0, 1, 2, 3, 5, 4, 6).reshape(
            count, 2, vectors, comps // 2, 2, edge // 2 * lanes
        )

    branches = [
        functools.partial(both, oz, oy)
        for oz in range(1, MAX_OFFSET + 1)
        for oy in range(1, MAX_OFFSET + 1)
    ]
    which = (offsets[1] - 1) * MAX_OFFSET + offsets[2] - 1
    return lax.switch(which, branches, offsets, slots, lattice)


ridge_scale = 0.05
top_precision = lax.Precision.HIGHEST


def from_behind(array, axis, by):
    length = lax.axis_size(axis)
    return lax.ppermute(array, axis, [(i, (i + by) % length) for i in range(length)])


def factor_pass(blocks):
    norm_count = blocks.shape[3] * blocks.shape[5]
    products = (
        jnp.einsum("nkvcas,nkwcbs->nkavbw", blocks, blocks, precision=top_precision) / norm_count
    )
    gram_real = products[:, :, 0, :, 0, :] + products[:, :, 1, :, 1, :]
    gram_imag = products[:, :, 0, :, 1, :] - products[:, :, 1, :, 0, :]
    width = gram_real.shape[-1]
    diag_mean = jnp.mean(jnp.diagonal(gram_real, axis1=2, axis2=3), axis=-1)
    ridge_term = ridge_scale * (diag_mean + 1e-06)
    gram_real = jnp.moveaxis(gram_real, (2, 3), (0, 1))
    gram_imag = jnp.moveaxis(gram_imag, (2, 3), (0, 1))
    zero_batch = jnp.zeros_like(ridge_term)
    low_real = [[zero_batch] * width for row_idx in range(width)]
    low_imag = [[zero_batch] * width for row_idx in range(width)]
    for col_idx in range(width):
        remain = gram_real[col_idx, col_idx] + ridge_term
        for mid_idx in range(col_idx):
            remain = remain - low_real[col_idx][mid_idx] * low_real[col_idx][mid_idx]
            remain = remain - low_imag[col_idx][mid_idx] * low_imag[col_idx][mid_idx]
        diag_val = jnp.sqrt(remain)
        low_real[col_idx][col_idx] = diag_val
        for row_idx in range(col_idx + 1, width):
            sum_real = gram_real[row_idx, col_idx]
            sum_imag = gram_imag[row_idx, col_idx]
            for mid_idx in range(col_idx):
                left_real = low_real[row_idx][mid_idx]
                left_imag = low_imag[row_idx][mid_idx]
                right_real = low_real[col_idx][mid_idx]
                right_imag = low_imag[col_idx][mid_idx]
                sum_real = sum_real - (left_real * right_real + left_imag * right_imag)
                sum_imag = sum_imag - (left_imag * right_real - left_real * right_imag)
            low_real[row_idx][col_idx] = sum_real / diag_val
            low_imag[row_idx][col_idx] = sum_imag / diag_val
    inv_real = [[zero_batch] * width for row_idx in range(width)]
    inv_imag = [[zero_batch] * width for row_idx in range(width)]
    for col_idx in range(width):
        inv_real[col_idx][col_idx] = 1.0 / low_real[col_idx][col_idx]
        for row_idx in range(col_idx + 1, width):
            sum_real = zero_batch
            sum_imag = zero_batch
            for mid_idx in range(col_idx, row_idx):
                left_real = low_real[row_idx][mid_idx]
                left_imag = low_imag[row_idx][mid_idx]
                right_real = inv_real[mid_idx][col_idx]
                right_imag = inv_imag[mid_idx][col_idx]
                sum_real = sum_real + left_real * right_real - left_imag * right_imag
                sum_imag = sum_imag + left_real * right_imag + left_imag * right_real
            inv_real[row_idx][col_idx] = -sum_real / low_real[row_idx][row_idx]
            inv_imag[row_idx][col_idx] = -sum_imag / low_real[row_idx][row_idx]
    map_real = jnp.stack(
        [
            jnp.stack([inv_real[w_idx][v_idx] for w_idx in range(width)], axis=-1)
            for v_idx in range(width)
        ],
        axis=-2,
    )
    map_imag = -jnp.stack(
        [
            jnp.stack([inv_imag[w_idx][v_idx] for w_idx in range(width)], axis=-1)
            for v_idx in range(width)
        ],
        axis=-2,
    )
    mixing = jnp.stack(
        [jnp.stack([map_real, map_imag], axis=3), jnp.stack([-map_imag, map_real], axis=3)], axis=2
    )
    return jnp.einsum("nkvcas,nkavbw->nkwcbs", blocks, mixing, precision=top_precision)


def two_passes(blocks):
    return factor_pass(factor_pass(blocks))


def arrange(lattice, row_count, agg_edge):
    vector_count = lattice.shape[3]
    comp_count = lattice.shape[4]
    x_sites = lattice.shape[6]
    groups = x_sites // agg_edge
    pieces = lattice.reshape(
        row_count, agg_edge, agg_edge, vector_count, 2, comp_count // 2, 2, groups, agg_edge
    )
    pieces = pieces.transpose(7, 4, 3, 5, 6, 0, 1, 2, 8)
    return pieces.reshape(
        groups, 2, vector_count, comp_count // 2, 2, row_count * agg_edge * agg_edge * agg_edge
    )


def invert(slot_row):
    places = jnp.arange(slot_row.shape[0], dtype=jnp.int32)
    return jnp.sum(jnp.where(slot_row[None, :] == places[:, None], places[None, :], 0), axis=1)


def per_device_general(near_null, offsets, owner_slot):
    agg_edge = near_null.shape[0]
    rim_rows = agg_edge - 1
    from_z = from_behind(near_null[:, :rim_rows], "gz", -1)
    lattice = lax.dynamic_slice_in_dim(
        jnp.concatenate([near_null, from_z], axis=1), offsets[1], agg_edge, 1
    )
    from_y = from_behind(lattice[:, :, :rim_rows], "gy", -1)
    lattice = lax.dynamic_slice_in_dim(
        jnp.concatenate([lattice, from_y], axis=2), offsets[2], agg_edge, 2
    )
    x_sites = lattice.shape[5] // 2
    lattice = lattice.reshape(lattice.shape[:5] + (2, x_sites))
    lattice = lax.dynamic_slice_in_dim(
        jnp.concatenate([lattice, lattice], axis=6), offsets[3], x_sites, 6
    )
    slot_row = owner_slot.reshape(-1)
    source_of = invert(slot_row)
    from_t = from_behind(lattice[:rim_rows], "ta", -1)
    lattice = lax.dynamic_slice_in_dim(
        jnp.concatenate([lattice, from_t], axis=0), offsets[0], agg_edge, 0
    )
    tiles = arrange(lattice, agg_edge, agg_edge)
    packed = jnp.take(tiles, source_of, axis=0)
    result = two_passes(lax.all_to_all(packed, "ta", split_axis=0, concat_axis=0, tiled=True))
    return result


def solution(mesh):
    pair = mesh.shape["ta"] == 2 and mesh.shape["gz"] > 1 and mesh.shape["gy"] > 1
    return jax.shard_map(
        per_device_pair if pair else per_device_general,
        mesh=mesh,
        in_specs=(P("ta", "gz", "gy", None, None, None), P(), P("ta", "gz", "gy", None)),
        out_specs=P(("ta", "gz", "gy"), None, None, None, None, None),
        check_vma=False,
    )
```
